32 devices in a mesh: rows: 8 (over z, x), cols: 4 (over y, core).
Axes of the slice: x: 2, y: 2, z: 4, core: 2. Of those that a mesh axis runs over, the one named last changes fastest.
Arguments:
- left_features: bfloat16 [2, 96, 512, 256], P(None, 'rows', 'cols'), may hold values from -6 to 6
- right_features: bfloat16 [2, 96, 512, 256], P(None, 'rows', 'cols'), may hold values from -6 to 6
- conv_weight: bfloat16 [3, 3, 256, 256], replicated, may hold values from -0.125 to 0.125
- conv_bias: float32 [256], replicated, may hold values from -3 to 3
Outputs:
- pyramid_out: float32 [2, 96, 512, 480], P(None, 'rows', 'cols')
The draws below stay inside these ranges and needn't reach their ends.
All inputs are finite; a program needn't handle non-finite values.
Results may differ from the reference program's by a relative error of at most 0.0012.
Values may be sent and summed in bfloat16 or wider, within the bound.
A program may use at most 64 MiB of HBM per device.

```python
import math
import jax
import jax.numpy as jnp
from jax import lax

C = 256
DISP = 256
LEVELS = 4
B = 2
H_FEAT = 96
W_FEAT = 512


def steps_of(own_key, dims, pieces, low, largest):
    loudness, own = 1.0, jax.random.fold_in(own_key, 6)
    for position, shards_of in pieces:
        heights = jnp.exp(jax.random.uniform(jax.random.fold_in(own, position), (shards_of,), jnp.float32, low / len(pieces), largest / len(pieces)))
        loudness = loudness * jnp.repeat(heights, dims[position] // shards_of).reshape([-1 if axis == position else 1 for axis in range(len(dims))])
    return loudness


def noise(stream_key, extent, spread, reach, pieces=(), held_as=jnp.bfloat16):
    values = spread * jax.random.normal(stream_key, extent, jnp.float32)
    if pieces:
        values = values * steps_of(stream_key, extent, pieces, -0.22, 0.18)
    return jnp.clip(values, -reach, reach).astype(held_as)


def setup_inputs(seed: int = 0) -> dict:
    seeds = jax.random.split(jax.random.key(seed), 5)
    left_features = noise(seeds[0], (B, H_FEAT, W_FEAT, C), 1.0, 6.0, ((1, 8), (2, 4)))
    right_features = noise(seeds[1], (B, H_FEAT, W_FEAT, C), 1.0, 6.0, ((1, 8), (2, 4)))
    conv_weight = noise(seeds[2], (3, 3, C, C), (9 * C) ** -0.5, 0.125)
    conv_bias = noise(seeds[3], (C,), 0.5, 3.0, (), jnp.float32)
    return {"left_features": left_features, "right_features": right_features, "conv_weight": conv_weight, "conv_bias": conv_bias}


def conv_block(picture, conv_weight, conv_bias):
    height = picture.shape[0] - 2
    breadth = picture.shape[1] - 2
    channels = picture.shape[2]
    total = jnp.zeros((height * breadth, channels), jnp.float32)
    for row_tap in range(3):
        for col_tap in range(3):
            window = picture[row_tap:row_tap + height, col_tap:col_tap + breadth].reshape(-1, channels)
            total = total + jnp.dot(window, conv_weight[row_tap, col_tap], preferred_element_type=jnp.float32)
    centre = picture[1:-1, 1:-1].reshape(-1, channels).astype(jnp.float32)
    encoded = centre + jax.nn.relu(total + conv_bias.astype(jnp.float32))
    return encoded.astype(jnp.bfloat16).reshape(height, breadth, channels)

def pyramid(scores, span_count, level_count, channels):
    queries = scores.shape[-2]
    across = scores.shape[-1]
    leading = scores.shape[:-2]
    skewed = scores[..., 1:].reshape(leading + (-1,))
    skewed = jnp.pad(skewed, [(0, 0)] * len(leading) + [(0, queries)])
    skewed = skewed.reshape(leading + (queries, across))[..., :span_count][..., ::-1]
    volume = skewed * (1.0 / math.sqrt(channels))
    levels = [volume]
    for level in range(1, level_count):
        pooled = volume.reshape(leading + (queries, span_count >> level, 1 << level)).mean(axis=-1)
        levels.append(pooled)
    return jnp.concatenate(levels, axis=-1)

def reference(left_features, right_features, conv_weight, conv_bias):
    batch, height, breadth, channels = left_features.shape

    def encode(images):
        padded = jnp.pad(images, ((0, 0), (1, 1), (1, 1), (0, 0)))
        return lax.map(lambda picture: conv_block(picture, conv_weight, conv_bias), padded)
    left_out = encode(left_features)
    right_out = encode(right_features)
    right_padded = jnp.pad(right_out, ((0, 0), (0, 0), (DISP, 0), (0, 0)))
    left_rows = left_out.reshape(batch * height, breadth, channels)
    right_rows = right_padded.reshape(batch * height, DISP + breadth, channels)

    def one_row(pair):
        scores = jnp.dot(pair[0], pair[1].T, preferred_element_type=jnp.float32)
        return pyramid(scores, DISP, LEVELS, channels)
    result = lax.map(one_row, (left_rows, right_rows))
    return result.reshape(batch, height, breadth, -1)
```

```python
import functools
import math

import jax
import jax.numpy as jnp
from jax import lax
from jax.experimental import pallas as pl
from jax.experimental.pallas import tpu as pltpu
from jax.sharding import PartitionSpec as P

DISP = 256
LEVELS = 4


MESH = pl.DeviceIdType.MESH
AROUND = ((-1, 0), (1, 0), (0, -1), (0, 1), (-1, -1), (-1, 1), (1, -1), (1, 1))
OPPOSITE = (1, 0, 3, 2, 7, 6, 5, 4)
ROW_SIDES = (0, 1)
COL_SIDES = (2, 3)
CORNERS = (4, 5, 6, 7)
LEFT, RIGHT = 0, 1


def kernel(
    row_count, col_count, part, span_count, level_count, scale,
    left, right, weight_hbm, bias_hbm, out,
    images, sides, edges, col_halo, weight, bias, enc, near, far, back, tri_out, tri_in, scores, stage,
    in_sems, send_sem, recv_sem, own_sems, far_sems, pass_sems, back_sems, tri_sems,
):
    batch, height, breadth, channels = left.shape
    my_row, my_col = lax.axis_index("rows"), lax.axis_index("cols")
    parts = height // part
    chunks = batch * parts
    inner = batch * max(parts - 2, 0)

    def inside(step_row, step_col):
        row, col = my_row + step_row, my_col + step_col
        return (row >= 0) & (row < row_count) & (col >= 0) & (col < col_count)

    odd = lax.rem(my_col, 2) == 1
    even = jnp.logical_not(odd)
    has_two = my_col >= 2
    gives_two = my_col + 2 < col_count
    has_near = my_col >= 1
    first = jnp.where(gives_two, RIGHT, LEFT)
    second = 1 - first

    def fetch(image):
        source = right if image == RIGHT else left
        return pltpu.make_async_copy(
            source, images.at[image, :, pl.ds(1, height)], in_sems.at[image]
        )

    def fetch_weight():
        return pltpu.make_async_copy(weight_hbm, weight, in_sems.at[2])

    def fetch_bias():
        return pltpu.make_async_copy(bias_hbm, bias, in_sems.at[3])

    for image in (RIGHT, LEFT):

        @pl.when(first == image)
        def _():
            fetch(image).start()
            fetch_weight().start()
            fetch_bias().start()
            fetch(1 - image).start()

    barrier = pltpu.get_barrier_semaphore()
    partners = AROUND + ((0, -2), (0, 2))
    for step_row, step_col in partners:

        @pl.when(inside(step_row, step_col))
        def _():
            pl.semaphore_signal(
                barrier, inc=1, device_id=(my_row + step_row, my_col + step_col), device_id_type=MESH
            )

    def halo_copy(side, image):
        step_row, step_col = AROUND[side]
        if step_col == 0:
            source = images.at[image, :, 1 if step_row < 0 else height]
            target = images.at[image, :, height + 1 if step_row < 0 else 0]
        else:
            mine, theirs = (0, 1) if step_col < 0 else (1, 0)
            if step_row == 0:
                source = edges.at[mine, image]
                target = col_halo.at[theirs, image, :, pl.ds(1, height)]
            else:
                source = edges.at[mine, image, :, 0 if step_row < 0 else height - 1]
                target = col_halo.at[theirs, image, :, height + 1 if step_row < 0 else 0]
        return pltpu.make_async_remote_copy(
            src_ref=source, dst_ref=target,
            send_sem=send_sem.at[image, side], recv_sem=recv_sem.at[image, OPPOSITE[side]],
            device_id=(my_row + step_row, my_col + step_col), device_id_type=MESH,
        )

    def take_edges(image):
        def line(i, carry):
            b, h = i // height, lax.rem(i, height)
            low = images[image, b, h + 1, 0:16].astype(jnp.float32)
            high = images[image, b, h + 1, breadth - 16 : breadth].astype(jnp.float32)
            edges[0, image, b, h] = low[0:1]
            edges[1, image, b, h] = high[15:16]
            return carry

        lax.fori_loop(0, batch * height, line, 0)

    def send_halo(which, image):
        for side in which:

            @pl.when(inside(*AROUND[side]))
            def _():
                halo_copy(side, image).start()

    def wait_halo(which, image):
        for side in which:

            @pl.when(inside(*AROUND[OPPOSITE[side]]))
            def _():
                halo_copy(side, image).wait_recv()

    def clear_halo():
        for side in range(8):
            step_row, step_col = AROUND[side]

            @pl.when(jnp.logical_not(inside(step_row, step_col)))
            def _():
                line = 0 if step_row < 0 else height + 1
                for image in (LEFT, RIGHT):
                    for b in range(batch):
                        if step_col == 0:
                            images[image, b, line] = jnp.zeros((breadth, channels), jnp.bfloat16)
                        elif step_row == 0:
                            col_halo[0 if step_col < 0 else 1, image, b, pl.ds(1, height)] = jnp.zeros(
                                (height, 1, channels), jnp.float32
                            )
                        else:
                            col_halo[0 if step_col < 0 else 1, image, b, line] = jnp.zeros(
                                (1, channels), jnp.float32
                            )

    for image in (RIGHT, LEFT):

        @pl.when(first == image)
        def _():
            fetch(image).wait()

    take_edges(first)
    peers = sum(inside(*step).astype(jnp.int32) for step in partners)
    pl.semaphore_wait(barrier, peers)
    for image in (RIGHT, LEFT):

        @pl.when(first == image)
        def _():
            send_halo(COL_SIDES + CORNERS, image)
            fetch(1 - image).wait()

    take_edges(second)
    for image in (RIGHT, LEFT):

        @pl.when(first == image)
        def _():
            send_halo(COL_SIDES + CORNERS, 1 - image)
            send_halo(ROW_SIDES, image)

    clear_halo()

    @pl.when(jnp.logical_not(has_near))
    def _():
        near[...] = jnp.zeros_like(near)

    @pl.when(jnp.logical_not(has_two))
    def _():
        scores[:, 2 * breadth :] = jnp.zeros((part, scores.shape[1] - 2 * breadth, breadth), jnp.float32)

    fetch_weight().wait()
    fetch_bias().wait()

    column = lax.broadcasted_iota(jnp.int32, (breadth, 1), 0)
    flip = jnp.where(
        lax.broadcasted_iota(jnp.int32, (breadth, breadth), 0)
        + lax.broadcasted_iota(jnp.int32, (breadth, breadth), 1)
        == breadth - 1,
        1.0, 0.0,
    ).astype(jnp.bfloat16)

    def place_of(step):
        after = step - inner
        is_inner = step < inner
        span = max(parts - 2, 1)
        b = jnp.where(is_inner, step // span, lax.rem(jnp.maximum(after, 0), batch))
        c = jnp.where(
            is_inner, 1 + lax.rem(step, span), (jnp.maximum(after, 0) // batch) * (parts - 1)
        )
        return b, c * part

    def chunk(step):
        b, h = place_of(step)
        return pl.ds(b * height + h, part)

    def remote(source, target, sems, step, away):
        return pltpu.make_async_remote_copy(
            src_ref=source.at[chunk(step)], dst_ref=target.at[chunk(step)],
            send_sem=sems.at[0, step], recv_sem=sems.at[1, step],
            device_id=(my_row, my_col + away), device_id_type=MESH,
        )

    def own_copy(step):
        return remote(enc.at[RIGHT], near, own_sems, step, 1)

    def far_copy(step):
        return remote(enc.at[RIGHT], far, far_sems, step, 2)

    def pass_copy(step):
        return remote(far, near, pass_sems, step, -1)

    def back_copy(step):
        return remote(enc.at[LEFT], back, back_sems, step, -2)

    def tri_copy(step):
        return remote(tri_out, tri_in, tri_sems, step, 2)

    def convolve(image, step):
        b, h = place_of(step)
        for line in range(part + 2):
            row = images[image, b, h + line].astype(jnp.float32)
            before = col_halo[0, image, b, h + line]
            after = col_halo[1, image, b, h + line]
            sides[line, :, :channels] = jnp.where(
                column == 0, before, pltpu.roll(row, 1, 0)
            ).astype(jnp.bfloat16)
            sides[line, :, channels:] = jnp.where(
                column == breadth - 1, after, pltpu.roll(row, breadth - 1, 0)
            ).astype(jnp.bfloat16)
        pieces = []
        for tap in range(3):
            beside = sides[tap : tap + part].reshape(part * breadth, 2 * channels)
            centre = images[image, b, pl.ds(h + tap, part)].reshape(part * breadth, channels)
            pieces += [beside[:, :channels], centre, beside[:, channels:]]
        total = jnp.dot(
            jnp.concatenate(pieces, axis=1), weight[...], preferred_element_type=jnp.float32
        ) + bias[...]
        centre = images[image, b, pl.ds(h + 1, part)].reshape(part * breadth, channels)
        result = centre.astype(jnp.float32) + jnp.maximum(total, 0.0)
        result = result.astype(jnp.bfloat16).reshape(part, breadth, channels)
        base = b * height + h

        @pl.when(image == LEFT)
        def _():
            enc[LEFT, pl.ds(base, part)] = result

            @pl.when(even & has_two)
            def _():
                back_copy(step).start()

        @pl.when(image == RIGHT)
        def _():
            for row in range(part):
                turned = jnp.dot(flip, result[row], preferred_element_type=jnp.float32)
                enc[RIGHT, base + row] = turned.astype(jnp.bfloat16)

            @pl.when(even)
            def _():
                own_copy(step).start()

            @pl.when(odd & gives_two)
            def _():
                far_copy(step).start()

    def conv_loop(image, low, high):
        def body(step, carry):
            convolve(image, step)
            return carry

        lax.fori_loop(low, high, body, 0)

    def both(act, image):
        for choice in (RIGHT, LEFT):

            @pl.when(image == choice)
            def _():
                act(choice)

    both(functools.partial(wait_halo, COL_SIDES), first)
    if inner:
        conv_loop(first, 0, inner)
    both(functools.partial(wait_halo, ROW_SIDES + CORNERS), first)
    both(functools.partial(send_halo, ROW_SIDES), second)
    conv_loop(first, inner, chunks)
    both(functools.partial(wait_halo, COL_SIDES), second)
    if inner:
        conv_loop(second, 0, inner)
    both(functools.partial(wait_halo, ROW_SIDES + CORNERS), second)
    conv_loop(second, inner, chunks)

    def product(keys, queries):
        return lax.dot_general(
            keys, queries, (((1,), (1,)), ((), ())), preferred_element_type=jnp.float32
        )

    blocks = breadth // 8
    lane8 = lax.broadcasted_iota(jnp.int32, (8, breadth), 1)

    def triangle(step, carry):
        b, h = place_of(step)
        base = b * height + h
        back_copy(step).wait_recv()
        for row in range(part):
            block = product(enc[RIGHT, base + row], back[base + row])
            tri_out[base + row, 0:8] = block[0:8]
            for i in range(1, blocks // 2):
                cut = breadth - 8 * i
                tri_out[base + row, 8 * i : 8 * i + 8] = jnp.where(
                    lane8 < cut, block[8 * i : 8 * i + 8], pltpu.roll(block[cut : cut + 8], cut, 1)
                )
            tri_out[base + row, breadth // 2 :] = block[breadth // 2 : breadth // 2 + 8]
        tri_copy(step).start()
        return carry

    @pl.when(even & gives_two)
    def _():
        lax.fori_loop(0, chunks, triangle, 0)

    steps_right = breadth - 1 - lax.broadcasted_iota(jnp.int32, (1, breadth), 1)

    def volume_row(slot, line):
        bit = breadth // 2
        keep = span_count + bit
        value = None
        while bit >= 8:
            keep = span_count + bit
            if value is None:
                low, high = scores[slot, :keep], scores[slot, bit : bit + keep]
            else:
                low, high = value[:keep], value[bit : bit + keep]
            value = jnp.where((steps_right & bit) != 0, high, low)
            bit //= 2
        for index, bit in enumerate((4, 2, 1)):
            keep = span_count + (8 if bit > 1 else 0)
            stage[slot, index, : span_count + 8] = value
            value = jnp.where(
                (steps_right & bit) != 0, stage[slot, index, pl.ds(bit, keep)], value[:keep]
            )
        out[line, :span_count] = value * scale
        start, size = 0, span_count
        for _ in range(1, level_count):
            half = size // 2
            pooled = (
                out[line, pl.ds(start, half, stride=2)] + out[line, pl.ds(start + 1, half, stride=2)]
            ) * 0.5
            start, size = start + size, half
            out[line, start : start + half] = pooled

    def finish(step, carry):
        b, h = place_of(step)
        base = b * height + h

        @pl.when(odd)
        def _():
            own_copy(step).wait_recv()

        @pl.when(odd & has_two)
        def _():
            far_copy(step).wait_recv()
            pass_copy(step).start()
            for row in range(part):
                scores[row, 2 * breadth : 3 * breadth] = product(
                    far[base + row], enc[LEFT, base + row]
                )

        @pl.when(even & has_two)
        def _():
            pass_copy(step).wait_recv()
            tri_copy(step).wait_recv()
            for row in range(part):
                for i in range(blocks // 2 + 1):
                    block = tri_in[base + row, 8 * i : 8 * i + 8]
                    scores[row, 2 * breadth + 8 * i : 2 * breadth + 8 * i + 8] = block
                    if 0 < i < blocks // 2:
                        cut = breadth - 8 * i
                        scores[row, 2 * breadth + cut : 2 * breadth + cut + 8] = pltpu.roll(
                            block, 8 * i, 1
                        )

        for row in range(part):
            scores[row, :breadth] = product(enc[RIGHT, base + row], enc[LEFT, base + row])
            scores[row, breadth : 2 * breadth] = product(near[base + row], enc[LEFT, base + row])
            volume_row(row, base + row)
        return carry

    lax.fori_loop(0, chunks, finish, 0)

    def drain(step, carry):
        @pl.when(even)
        def _():
            own_copy(step).wait_send()

        @pl.when(odd & gives_two)
        def _():
            far_copy(step).wait_send()

        @pl.when(odd & has_two)
        def _():
            pass_copy(step).wait_send()

        @pl.when(even & has_two)
        def _():
            back_copy(step).wait_send()

        @pl.when(even & gives_two)
        def _():
            tri_copy(step).wait_send()

        return carry

    lax.fori_loop(0, chunks, drain, 0)
    for side in range(8):

        @pl.when(inside(*AROUND[side]))
        def _():
            for image in (LEFT, RIGHT):
                halo_copy(side, image).wait_send()


def in_hbm(array):
    return pltpu.with_memory_space_constraint(array, pltpu.HBM)


def shards(left_features, right_features, conv_weight, conv_bias):
    batch, height, breadth, channels = left_features.shape
    col_count = lax.axis_size("cols")
    assert 2 * breadth == DISP and col_count % 2 == 0 and breadth % 16 == 0
    part = math.gcd(height, 4)
    lines = batch * height
    chunks = lines // part
    width = sum(DISP >> level for level in range(LEVELS))
    hbm = pl.BlockSpec(memory_space=pltpu.HBM)
    vmem = pl.BlockSpec(memory_space=pltpu.VMEM)
    dma = pltpu.SemaphoreType.DMA
    bf16, f32 = jnp.bfloat16, jnp.float32
    tri_rows = breadth // 2 + 8
    out = pl.pallas_call(
        functools.partial(
            kernel, lax.axis_size("rows"), col_count, part, DISP, LEVELS, 1.0 / math.sqrt(channels)
        ),
        out_shape=jax.ShapeDtypeStruct((lines, width, breadth), f32),
        in_specs=[hbm] * 4,
        out_specs=vmem,
        scratch_shapes=[
            pltpu.VMEM((2, batch, height + 2, breadth, channels), bf16),
            pltpu.VMEM((part + 2, breadth, 2 * channels), bf16),
            pltpu.VMEM((2, 2, batch, height, 1, channels), f32),
            pltpu.VMEM((2, 2, batch, height + 2, 1, channels), f32),
            pltpu.VMEM((9 * channels, channels), bf16),
            pltpu.VMEM((1, channels), f32),
            pltpu.VMEM((2, lines, breadth, channels), bf16),
            pltpu.VMEM((lines, breadth, channels), bf16),
            pltpu.VMEM((lines, breadth, channels), bf16),
            pltpu.VMEM((lines, breadth, channels), bf16),
            pltpu.VMEM((lines, tri_rows, breadth), f32),
            pltpu.VMEM((lines, tri_rows, breadth), f32),
            pltpu.VMEM((part, 3 * breadth, breadth), f32),
            pltpu.VMEM((part, 3, DISP + 16, breadth), f32),
            dma((4,)), dma((2, 8)), dma((2, 8)),
            dma((2, chunks)), dma((2, chunks)), dma((2, chunks)), dma((2, chunks)), dma((2, chunks)),
        ],
        compiler_params=pltpu.CompilerParams(
            collective_id=0, has_side_effects=True, vmem_limit_bytes=40 * 2**20
        ),
    )(
        in_hbm(left_features), in_hbm(right_features),
        in_hbm(conv_weight.reshape(9 * channels, channels)), in_hbm(conv_bias.reshape(1, -1)),
    )
    return jnp.swapaxes(out, 1, 2).reshape(batch, height, breadth, -1)


def solution(mesh):
    return jax.shard_map(
        shards,
        mesh=mesh,
        in_specs=(P(None, "rows", "cols", None), P(None, "rows", "cols", None), P(), P()),
        out_specs=P(None, "rows", "cols", None),
        check_vma=False,
    )
```

```python
import functools
import math

import jax
import jax.numpy as jnp
from jax import lax
from jax.experimental import pallas as pl
from jax.experimental.pallas import tpu as pltpu
from jax.sharding import PartitionSpec as P

DISP = 256
LEVELS = 4


MESH = pl.DeviceIdType.MESH
AROUND = ((-1, 0), (1, 0), (0, -1), (0, 1), (-1, -1), (-1, 1), (1, -1), (1, 1))
OPPOSITE = (1, 0, 3, 2, 7, 6, 5, 4)
ROW_SIDES = (0, 1)
COL_SIDES = (2, 3)
CORNERS = (4, 5, 6, 7)
LEFT, RIGHT = 0, 1


def kernel(
    row_count, col_count, part, span_count, level_count, scale,
    left, right, weight_hbm, bias_hbm, out,
    images, sides, raw_edges, edges, col_halo, weight, bias, enc, near, far, back, tri_out, tri_in, scores, stage,
    in_sems, edge_sems, send_sem, recv_sem, own_sems, far_sems, pass_sems, back_sems, tri_sems,
):
    batch, height, breadth, channels = left.shape
    my_row, my_col = lax.axis_index("rows"), lax.axis_index("cols")
    edge = part // 2
    spans = height // part - 1
    chunks = batch * (spans + 1)
    inner = batch * spans

    def inside(step_row, step_col):
        row, col = my_row + step_row, my_col + step_col
        return (row >= 0) & (row < row_count) & (col >= 0) & (col < col_count)

    odd = lax.rem(my_col, 2) == 1
    even = jnp.logical_not(odd)
    has_two = my_col >= 2
    gives_two = my_col + 2 < col_count
    has_near = my_col >= 1
    first = jnp.where(gives_two, RIGHT, LEFT)
    second = 1 - first

    def fetch(image):
        source = right if image == RIGHT else left
        return pltpu.make_async_copy(
            source, images.at[image, :, pl.ds(1, height)], in_sems.at[image]
        )

    def fetch_edge(side, image):
        source = right if image == RIGHT else left
        return pltpu.make_async_copy(
            source.at[:, :, pl.ds(side * (breadth - 16), 16)],
            raw_edges.at[side, image], edge_sems.at[side, image],
        )

    def fetch_weight():
        return pltpu.make_async_copy(weight_hbm, weight, in_sems.at[2])

    def fetch_bias():
        return pltpu.make_async_copy(bias_hbm, bias, in_sems.at[3])

    barrier = pltpu.get_barrier_semaphore()
    partners = AROUND + ((0, -2), (0, 2))
    for step_row, step_col in partners:

        @pl.when(inside(step_row, step_col))
        def _():
            pl.semaphore_signal(
                barrier, inc=1, device_id=(my_row + step_row, my_col + step_col), device_id_type=MESH
            )

    for image in (RIGHT, LEFT):

        @pl.when(first == image)
        def _():
            for choice in (image, 1 - image):
                for side in range(2):
                    fetch_edge(side, choice).start()
            fetch(image).start()
            fetch_weight().start()
            fetch_bias().start()
            fetch(1 - image).start()

    def halo_copy(side, image):
        step_row, step_col = AROUND[side]
        if step_col == 0:
            source = images.at[image, :, 1 if step_row < 0 else height]
            target = images.at[image, :, height + 1 if step_row < 0 else 0]
        else:
            mine, theirs = (0, 1) if step_col < 0 else (1, 0)
            if step_row == 0:
                source = edges.at[mine, image]
                target = col_halo.at[theirs, image, :, pl.ds(1, height)]
            else:
                source = edges.at[mine, image, :, 0 if step_row < 0 else height - 1]
                target = col_halo.at[theirs, image, :, height + 1 if step_row < 0 else 0]
        return pltpu.make_async_remote_copy(
            src_ref=source, dst_ref=target,
            send_sem=send_sem.at[image, side], recv_sem=recv_sem.at[image, OPPOSITE[side]],
            device_id=(my_row + step_row, my_col + step_col), device_id_type=MESH,
        )

    def take_edges(image):
        def line(i, carry):
            b, h = i // height, lax.rem(i, height)
            edges[0, image, b, h] = raw_edges[0, image, b, h].astype(jnp.float32)[0:1]
            edges[1, image, b, h] = raw_edges[1, image, b, h].astype(jnp.float32)[15:16]
            return carry

        lax.fori_loop(0, batch * height, line, 0)

    def send_halo(which, image):
        for side in which:

            @pl.when(inside(*AROUND[side]))
            def _():
                halo_copy(side, image).start()

    def wait_halo(which, image):
        for side in which:

            @pl.when(inside(*AROUND[OPPOSITE[side]]))
            def _():
                halo_copy(side, image).wait_recv()

    def clear_halo():
        for side in range(8):
            step_row, step_col = AROUND[side]

            @pl.when(jnp.logical_not(inside(step_row, step_col)))
            def _():
                line = 0 if step_row < 0 else height + 1
                for image in (LEFT, RIGHT):
                    for b in range(batch):
                        if step_col == 0:
                            images[image, b, line] = jnp.zeros((breadth, channels), jnp.bfloat16)
                        elif step_row == 0:
                            col_halo[0 if step_col < 0 else 1, image, b, pl.ds(1, height)] = jnp.zeros(
                                (height, 1, channels), jnp.float32
                            )
                        else:
                            col_halo[0 if step_col < 0 else 1, image, b, line] = jnp.zeros(
                                (1, channels), jnp.float32
                            )

    for image in (RIGHT, LEFT):

        @pl.when(first == image)
        def _():
            for side in range(2):
                fetch_edge(side, image).wait()

    take_edges(first)
    peers = sum(inside(*step).astype(jnp.int32) for step in partners)
    pl.semaphore_wait(barrier, peers)
    for image in (RIGHT, LEFT):

        @pl.when(first == image)
        def _():
            send_halo(COL_SIDES + CORNERS, image)
            for side in range(2):
                fetch_edge(side, 1 - image).wait()

    take_edges(second)
    for image in (RIGHT, LEFT):

        @pl.when(first == image)
        def _():
            send_halo(COL_SIDES + CORNERS, 1 - image)
            fetch(image).wait()
            send_halo(ROW_SIDES, image)
            fetch(1 - image).wait()
            send_halo(ROW_SIDES, 1 - image)

    clear_halo()

    @pl.when(jnp.logical_not(has_near))
    def _():
        near[...] = jnp.zeros_like(near)

    @pl.when(jnp.logical_not(has_two))
    def _():
        scores[:, 2 * breadth :] = jnp.zeros((part, scores.shape[1] - 2 * breadth, breadth), jnp.float32)

    fetch_weight().wait()
    fetch_bias().wait()

    column = lax.broadcasted_iota(jnp.int32, (breadth, 1), 0)
    flip = jnp.where(
        lax.broadcasted_iota(jnp.int32, (breadth, breadth), 0)
        + lax.broadcasted_iota(jnp.int32, (breadth, breadth), 1)
        == breadth - 1,
        1.0, 0.0,
    ).astype(jnp.bfloat16)

    def place_of(step, row):
        is_inner = step < inner
        b = jnp.where(is_inner, step // spans, step - inner)
        h = jnp.where(
            is_inner,
            edge + lax.rem(step, spans) * part + row,
            row if row < edge else height - part + row,
        )
        return b, h

    def remote(source, target, sems, step, away, rows=part):
        lines = pl.ds(step * rows, rows)
        return pltpu.make_async_remote_copy(
            src_ref=source.at[lines], dst_ref=target.at[lines],
            send_sem=sems.at[0, step], recv_sem=sems.at[1, step],
            device_id=(my_row, my_col + away), device_id_type=MESH,
        )

    def own_copy(step):
        return remote(enc.at[RIGHT], near, own_sems, step, 1)

    def far_copy(step):
        return remote(enc.at[RIGHT], far, far_sems, step, 2)

    def pass_copy(step):
        return remote(far, near, pass_sems, step, -1)

    def back_copy(step):
        return remote(enc.at[LEFT], back, back_sems, step, -2)

    def tri_copy(step):
        return remote(tri_out, tri_in, tri_sems, step, 2, part // 2)

    def convolve(image, step, b, starts, count):
        slots = count + 2
        for piece, start in enumerate(starts):
            for line in range(slots):
                row = images[image, b, start + line].astype(jnp.float32)
                before = col_halo[0, image, b, start + line]
                after = col_halo[1, image, b, start + line]
                sides[piece * slots + line, :, :channels] = jnp.where(
                    column == 0, before, pltpu.roll(row, 1, 0)
                ).astype(jnp.bfloat16)
                sides[piece * slots + line, :, channels:] = jnp.where(
                    column == breadth - 1, after, pltpu.roll(row, breadth - 1, 0)
                ).astype(jnp.bfloat16)

        def rows_from(offset):
            taken = [images[image, b, pl.ds(start + offset, count)] for start in starts]
            return jnp.concatenate(taken, axis=0).reshape(part * breadth, channels)

        pieces = []
        for tap in range(3):
            beside = jnp.concatenate(
                [sides[i * slots + tap : i * slots + tap + count] for i in range(len(starts))], axis=0
            ).reshape(part * breadth, 2 * channels)
            pieces += [beside[:, :channels], rows_from(tap), beside[:, channels:]]
        total = jnp.dot(
            jnp.concatenate(pieces, axis=1), weight[...], preferred_element_type=jnp.float32
        ) + bias[...]
        result = rows_from(1).astype(jnp.float32) + jnp.maximum(total, 0.0)
        result = result.astype(jnp.bfloat16).reshape(part, breadth, channels)
        base = step * part

        @pl.when(image == LEFT)
        def _():
            enc[LEFT, pl.ds(base, part)] = result

            @pl.when(even & has_two)
            def _():
                back_copy(step).start()

        @pl.when(image == RIGHT)
        def _():
            for row in range(part):
                turned = jnp.dot(flip, result[row], preferred_element_type=jnp.float32)
                enc[RIGHT, base + row] = turned.astype(jnp.bfloat16)

            @pl.when(even)
            def _():
                own_copy(step).start()

            @pl.when(odd & gives_two)
            def _():
                far_copy(step).start()

    def conv_inner(image):
        def body(step, carry):
            convolve(image, step, step // spans, [edge + lax.rem(step, spans) * part], part)
            return carry

        lax.fori_loop(0, inner, body, 0)

    def conv_edge(image):
        def body(step, carry):
            convolve(image, step, step - inner, [0, height - edge], edge)
            return carry

        lax.fori_loop(inner, chunks, body, 0)

    def both(act, image):
        for choice in (RIGHT, LEFT):

            @pl.when(image == choice)
            def _():
                act(choice)

    def product(keys, queries):
        return lax.dot_general(
            keys, queries, (((1,), (1,)), ((), ())), preferred_element_type=jnp.float32
        )

    half_blocks = breadth // 16
    lane8 = lax.broadcasted_iota(jnp.int32, (8, breadth), 1)

    def triangle(step, carry):
        base = step * part
        back_copy(step).wait_recv()
        for pair in range(0, part, 2):
            two = [product(enc[RIGHT, base + row], back[base + row]) for row in (pair, pair + 1)]
            for i in range(half_blocks + 1):
                cut = breadth - 8 * i
                kept = []
                for block in two:
                    piece = block[8 * i : 8 * i + 8]
                    if 0 < i < half_blocks:
                        piece = jnp.where(lane8 < cut, piece, pltpu.roll(block[cut : cut + 8], cut, 1))
                    kept.append(piece)
                tri_out[(base + pair) // 2, i] = jnp.concatenate(kept, axis=0).astype(jnp.bfloat16)
        tri_copy(step).start()
        return carry

    def triangles(low, high):
        @pl.when(even & gives_two)
        def _():
            lax.fori_loop(low, high, triangle, 0)

    both(functools.partial(wait_halo, COL_SIDES), first)
    conv_inner(first)
    both(functools.partial(wait_halo, COL_SIDES), second)
    conv_inner(second)
    both(functools.partial(wait_halo, ROW_SIDES + CORNERS), first)
    conv_edge(first)
    triangles(0, inner)
    both(functools.partial(wait_halo, ROW_SIDES + CORNERS), second)
    conv_edge(second)
    triangles(inner, chunks)

    steps_right = breadth - 1 - lax.broadcasted_iota(jnp.int32, (1, breadth), 1)

    def volume_row(slot, line):
        bit = breadth // 2
        keep = span_count + bit
        value = None
        while bit >= 8:
            keep = span_count + bit
            if value is None:
                low, high = scores[slot, :keep], scores[slot, bit : bit + keep]
            else:
                low, high = value[:keep], value[bit : bit + keep]
            value = jnp.where((steps_right & bit) != 0, high, low)
            bit //= 2
        for index, bit in enumerate((4, 2, 1)):
            keep = span_count + (8 if bit > 1 else 0)
            stage[slot, index, : span_count + 8] = value
            value = jnp.where(
                (steps_right & bit) != 0, stage[slot, index, pl.ds(bit, keep)], value[:keep]
            )
        out[line, :span_count] = value * scale
        start, size = 0, span_count
        for _ in range(1, level_count):
            half = size // 2
            pooled = (
                out[line, pl.ds(start, half, stride=2)] + out[line, pl.ds(start + 1, half, stride=2)]
            ) * 0.5
            start, size = start + size, half
            out[line, start : start + half] = pooled

    def finish(step, carry):
        base = step * part

        @pl.when(odd)
        def _():
            own_copy(step).wait_recv()

        @pl.when(odd & has_two)
        def _():
            far_copy(step).wait_recv()
            pass_copy(step).start()
            for row in range(part):
                scores[row, 2 * breadth : 3 * breadth] = product(
                    far[base + row], enc[LEFT, base + row]
                )

        @pl.when(even & has_two)
        def _():
            pass_copy(step).wait_recv()
            tri_copy(step).wait_recv()
            for pair in range(0, part, 2):
                for i in range(half_blocks + 1):
                    both_rows = tri_in[(base + pair) // 2, i].astype(jnp.float32)
                    for row in range(2):
                        block = both_rows[8 * row : 8 * row + 8]
                        start = 2 * breadth + 8 * i
                        scores[pair + row, start : start + 8] = block
                        if 0 < i < half_blocks:
                            start = 3 * breadth - 8 * i
                            scores[pair + row, start : start + 8] = pltpu.roll(block, 8 * i, 1)

        for row in range(part):
            scores[row, :breadth] = product(enc[RIGHT, base + row], enc[LEFT, base + row])
            scores[row, breadth : 2 * breadth] = product(near[base + row], enc[LEFT, base + row])
            b, h = place_of(step, row)
            volume_row(row, b * height + h)
        return carry

    lax.fori_loop(0, chunks, finish, 0)

    def drain(step, carry):
        @pl.when(even)
        def _():
            own_copy(step).wait_send()

        @pl.when(odd & gives_two)
        def _():
            far_copy(step).wait_send()

        @pl.when(odd & has_two)
        def _():
            pass_copy(step).wait_send()

        @pl.when(even & has_two)
        def _():
            back_copy(step).wait_send()

        @pl.when(even & gives_two)
        def _():
            tri_copy(step).wait_send()

        return carry

    lax.fori_loop(0, chunks, drain, 0)
    for side in range(8):

        @pl.when(inside(*AROUND[side]))
        def _():
            for image in (LEFT, RIGHT):
                halo_copy(side, image).wait_send()


def in_hbm(array):
    return pltpu.with_memory_space_constraint(array, pltpu.HBM)


def shards(left_features, right_features, conv_weight, conv_bias):
    batch, height, breadth, channels = left_features.shape
    col_count = lax.axis_size("cols")
    part = math.gcd(height, 4)
    assert 2 * breadth == DISP and col_count % 2 == 0 and breadth % 16 == 0
    assert part % 2 == 0 and height > part
    lines = batch * height
    chunks = lines // part
    width = sum(DISP >> level for level in range(LEVELS))
    hbm = pl.BlockSpec(memory_space=pltpu.HBM)
    vmem = pl.BlockSpec(memory_space=pltpu.VMEM)
    dma = pltpu.SemaphoreType.DMA
    bf16, f32 = jnp.bfloat16, jnp.float32
    tri = (lines // 2, breadth // 16 + 1, 16, breadth)
    out = pl.pallas_call(
        functools.partial(
            kernel, lax.axis_size("rows"), col_count, part, DISP, LEVELS, 1.0 / math.sqrt(channels)
        ),
        out_shape=jax.ShapeDtypeStruct((lines, width, breadth), f32),
        in_specs=[hbm] * 4,
        out_specs=vmem,
        scratch_shapes=[
            pltpu.VMEM((2, batch, height + 2, breadth, channels), bf16),
            pltpu.VMEM((part + 4, breadth, 2 * channels), bf16),
            pltpu.VMEM((2, 2, batch, height, 16, channels), bf16),
            pltpu.VMEM((2, 2, batch, height, 1, channels), f32),
            pltpu.VMEM((2, 2, batch, height + 2, 1, channels), f32),
            pltpu.VMEM((9 * channels, channels), bf16),
            pltpu.VMEM((1, channels), f32),
            pltpu.VMEM((2, lines, breadth, channels), bf16),
            pltpu.VMEM((lines, breadth, channels), bf16),
            pltpu.VMEM((lines, breadth, channels), bf16),
            pltpu.VMEM((lines, breadth, channels), bf16),
            pltpu.VMEM(tri, bf16),
            pltpu.VMEM(tri, bf16),
            pltpu.VMEM((part, 3 * breadth, breadth), f32),
            pltpu.VMEM((part, 3, DISP + 16, breadth), f32),
            dma((4,)), dma((2, 2)), dma((2, 8)), dma((2, 8)),
            dma((2, chunks)), dma((2, chunks)), dma((2, chunks)), dma((2, chunks)), dma((2, chunks)),
        ],
        compiler_params=pltpu.CompilerParams(
            collective_id=0, has_side_effects=True, vmem_limit_bytes=40 * 2**20
        ),
    )(
        in_hbm(left_features), in_hbm(right_features),
        in_hbm(conv_weight.reshape(9 * channels, channels)), in_hbm(conv_bias.reshape(1, -1)),
    )
    return jnp.swapaxes(out, 1, 2).reshape(batch, height, breadth, -1)


def solution(mesh):
    return jax.shard_map(
        shards,
        mesh=mesh,
        in_specs=(P(None, "rows", "cols", None), P(None, "rows", "cols", None), P(), P()),
        out_specs=P(None, "rows", "cols", None),
        check_vma=False,
    )
```

```python
import functools
import math

import jax
import jax.numpy as jnp
from jax import lax
from jax.experimental import pallas as pl
from jax.experimental.pallas import tpu as pltpu
from jax.sharding import PartitionSpec as P

DISP = 256
LEVELS = 4


MESH = pl.DeviceIdType.MESH
AROUND = ((-1, 0), (1, 0), (0, -1), (0, 1), (-1, -1), (-1, 1), (1, -1), (1, 1))
OPPOSITE = (1, 0, 3, 2, 7, 6, 5, 4)
ROW_SIDES = (0, 1)
COL_SIDES = (2, 3)
CORNERS = (4, 5, 6, 7)
LEFT, RIGHT, AHEAD = 0, 1, 2


def volume_row(scores, stage, out, slot, line, span_count, level_count, scale):
    breadth = scores.shape[2]
    steps = breadth - 1 - lax.broadcasted_iota(jnp.int32, (1, breadth), 1)
    bit = breadth // 2
    value = None
    while bit >= 8:
        keep = span_count + bit
        if value is None:
            low, high = scores[slot, :keep], scores[slot, bit : bit + keep]
        else:
            low, high = value[:keep], value[bit : bit + keep]
        value = jnp.where((steps & bit) != 0, high, low)
        bit //= 2
    for index, bit in enumerate((4, 2, 1)):
        keep = span_count + (8 if bit > 1 else 0)
        stage[slot, index, : span_count + 8] = value
        value = jnp.where((steps & bit) != 0, stage[slot, index, pl.ds(bit, keep)], value[:keep])
    out[line, :span_count] = value * scale
    start, size = 0, span_count
    for _ in range(1, level_count):
        half = size // 2
        pooled = (
            out[line, pl.ds(start, half, stride=2)] + out[line, pl.ds(start + 1, half, stride=2)]
        ) * 0.5
        start, size = start + size, half
        out[line, start : start + half] = pooled


def kernel(
    row_count, col_count, part, span_count, level_count, scale,
    left, right, weight_hbm, bias_hbm, out, held,
    images, sides, raw_edges, edges, col_halo, weight, bias, enc, near, far, back, tri_out, tri_in, scores, stage,
    in_sems, edge_sems, halo_sems, recv_sem, ahead_sems, send_sems, near_sems, two_sems, back_sems,
):
    batch, height, breadth, channels = left.shape
    my_row, my_col = lax.axis_index("rows"), lax.axis_index("cols")
    edge = part // 2
    spans = height // part - 1
    chunks = batch * (spans + 1)
    inner = batch * spans

    def inside(step_row, step_col):
        row, col = my_row + step_row, my_col + step_col
        return (row >= 0) & (row < row_count) & (col >= 0) & (col < col_count)

    odd = lax.rem(my_col, 2) == 1
    even = jnp.logical_not(odd)
    has_two = my_col >= 2
    gives_two = my_col + 2 < col_count
    has_near = my_col >= 1
    first = jnp.where(gives_two, RIGHT, LEFT)
    second = 1 - first

    def fetch(image):
        source = right if image == RIGHT else left
        return pltpu.make_async_copy(
            source, images.at[image, :, pl.ds(1, height)], in_sems.at[image]
        )

    def fetch_edge(side, image):
        source = right if image == RIGHT else left
        return pltpu.make_async_copy(
            source.at[:, :, pl.ds(side * (breadth - 16), 16)],
            raw_edges.at[side, image], edge_sems.at[side, image],
        )

    def fetch_weight():
        return pltpu.make_async_copy(weight_hbm, weight, in_sems.at[2])

    def fetch_bias():
        return pltpu.make_async_copy(bias_hbm, bias, in_sems.at[3])

    barrier = pltpu.get_barrier_semaphore()
    partners = AROUND + ((0, -2), (0, 2))
    for step_row, step_col in partners:

        @pl.when(inside(step_row, step_col))
        def _():
            pl.semaphore_signal(
                barrier, inc=1, device_id=(my_row + step_row, my_col + step_col), device_id_type=MESH
            )

    for image in (RIGHT, LEFT):

        @pl.when(first == image)
        def _():
            for choice in (image, 1 - image):
                for side in range(2):
                    fetch_edge(side, choice).start()
            fetch(image).start()
            fetch_weight().start()
            fetch_bias().start()
            fetch(1 - image).start()

    def halo_copy(side, image):
        step_row, step_col = AROUND[side]
        if step_col == 0:
            source = images.at[image, :, 1 if step_row < 0 else height]
            target = images.at[image, :, height + 1 if step_row < 0 else 0]
        else:
            mine, theirs = (0, 1) if step_col < 0 else (1, 0)
            if step_row == 0:
                source = edges.at[mine, image]
                target = col_halo.at[theirs, image, :, pl.ds(1, height)]
            else:
                source = edges.at[mine, image, :, 0 if step_row < 0 else height - 1]
                target = col_halo.at[theirs, image, :, height + 1 if step_row < 0 else 0]
        return pltpu.make_async_remote_copy(
            src_ref=source, dst_ref=target,
            send_sem=halo_sems.at[side],
            recv_sem=recv_sem.at[image if isinstance(image, int) else 0, OPPOSITE[side]],
            device_id=(my_row + step_row, my_col + step_col), device_id_type=MESH,
        )

    def ahead_copy(which, image):
        lines = pl.ds(edge, part + 2)
        if which == 0:
            source, target = images.at[image, 0, lines], images.at[AHEAD, 0, lines]
        else:
            source, target = col_halo.at[:, image, 0, lines], col_halo.at[:, AHEAD, 0, lines]
        return pltpu.make_async_remote_copy(
            src_ref=source, dst_ref=target,
            send_sem=ahead_sems.at[0, which], recv_sem=ahead_sems.at[1, which],
            device_id=(my_row, my_col + (2 if image == RIGHT else -2)), device_id_type=MESH,
        )

    sends_ahead = ((RIGHT, odd & gives_two), (LEFT, even & has_two))
    takes_ahead = ((RIGHT, odd & has_two), (LEFT, even & gives_two))

    def send_ahead(which, image):
        for choice, when in sends_ahead:
            if choice == image:

                @pl.when(when)
                def _():
                    ahead_copy(which, choice).start()

    def take_edges(image):
        for b in range(batch):
            for h in range(height):
                edges[0, image, b, h] = raw_edges[0, image, b, h].astype(jnp.float32)[0:1]
                edges[1, image, b, h] = raw_edges[1, image, b, h].astype(jnp.float32)[15:16]

    def send_halo(which, image):
        for side in which:

            @pl.when(inside(*AROUND[side]))
            def _():
                halo_copy(side, image).start()

    def wait_halo(which, image):
        for side in which:

            @pl.when(inside(*AROUND[OPPOSITE[side]]))
            def _():
                halo_copy(side, image).wait_recv()

    def clear_halo():
        for side in range(8):
            step_row, step_col = AROUND[side]

            @pl.when(jnp.logical_not(inside(step_row, step_col)))
            def _():
                line = 0 if step_row < 0 else height + 1
                for image in (LEFT, RIGHT):
                    for b in range(batch):
                        if step_col == 0:
                            images[image, b, line] = jnp.zeros((breadth, channels), jnp.bfloat16)
                        elif step_row == 0:
                            col_halo[0 if step_col < 0 else 1, image, b, pl.ds(1, height)] = jnp.zeros(
                                (height, 1, channels), jnp.float32
                            )
                        else:
                            col_halo[0 if step_col < 0 else 1, image, b, line] = jnp.zeros(
                                (1, channels), jnp.float32
                            )

    for image in (RIGHT, LEFT):

        @pl.when(first == image)
        def _():
            for side in range(2):
                fetch_edge(side, image).wait()

    take_edges(first)
    peers = sum(inside(*step).astype(jnp.int32) for step in partners)
    pl.semaphore_wait(barrier, peers)
    for image in (RIGHT, LEFT):

        @pl.when(first == image)
        def _():
            send_halo(COL_SIDES + CORNERS, image)
            for side in range(2):
                fetch_edge(side, 1 - image).wait()

    take_edges(second)
    for image in (RIGHT, LEFT):

        @pl.when(first == image)
        def _():
            send_halo(COL_SIDES + CORNERS, 1 - image)
            fetch(image).wait()
            send_ahead(0, image)
            send_halo(ROW_SIDES, image)
            fetch(1 - image).wait()
            send_ahead(0, 1 - image)
            send_halo(ROW_SIDES, 1 - image)

    clear_halo()

    @pl.when(jnp.logical_not(has_near))
    def _():
        near[...] = jnp.zeros_like(near)

    @pl.when(jnp.logical_not(has_two))
    def _():
        for target in (scores, held):
            target[:, 2 * breadth :] = jnp.zeros((part, breadth, breadth), jnp.float32)

    fetch_weight().wait()
    fetch_bias().wait()

    column = lax.broadcasted_iota(jnp.int32, (breadth, 1), 0)
    flip = jnp.where(
        lax.broadcasted_iota(jnp.int32, (breadth, breadth), 0)
        + lax.broadcasted_iota(jnp.int32, (breadth, breadth), 1)
        == breadth - 1,
        1.0, 0.0,
    ).astype(jnp.bfloat16)

    def place_of(step, row):
        is_inner = step < inner
        b = jnp.where(is_inner, step // spans, step - inner)
        h = jnp.where(
            is_inner,
            edge + lax.rem(step, spans) * part + row,
            row if row < edge else height - part + row,
        )
        return b, h

    def remote(source, target, send, recv, step, away, rows=part):
        lines = pl.ds(step * rows, rows)
        return pltpu.make_async_remote_copy(
            src_ref=source.at[lines], dst_ref=target.at[lines],
            send_sem=send_sems.at[send], recv_sem=recv.at[step],
            device_id=(my_row, my_col + away), device_id_type=MESH,
        )

    def own_copy(step):
        return remote(enc.at[RIGHT], near, 0, near_sems, step, 1)

    def far_copy(step):
        return remote(enc.at[RIGHT], far, 0, two_sems, step, 2)

    def pass_copy(step):
        return remote(far, near, 1, near_sems, step, -1)

    def back_copy(step):
        return remote(enc.at[LEFT], back, 1, back_sems, step, -2)

    def tri_copy(step):
        return remote(tri_out, tri_in, 2, two_sems, step, 2, part // 2)

    def sent(source, target, send, first_line, away):
        lines = pl.ds(first_line, source.shape[0] - first_line)
        return pltpu.make_async_remote_copy(
            src_ref=source.at[lines], dst_ref=target.at[lines],
            send_sem=send_sems.at[send], recv_sem=near_sems.at[0],
            device_id=(my_row, my_col + away), device_id_type=MESH,
        )

    def convolve(image, step, b, starts, count):
        slots = count + 2
        for piece, start in enumerate(starts):
            for line in range(slots):
                row = images[image, b, start + line].astype(jnp.float32)
                before = col_halo[0, image, b, start + line]
                after = col_halo[1, image, b, start + line]
                sides[piece * slots + line, :, :channels] = jnp.where(
                    column == 0, before, pltpu.roll(row, 1, 0)
                ).astype(jnp.bfloat16)
                sides[piece * slots + line, :, channels:] = jnp.where(
                    column == breadth - 1, after, pltpu.roll(row, breadth - 1, 0)
                ).astype(jnp.bfloat16)

        def rows_from(offset):
            taken = [images[image, b, pl.ds(start + offset, count)] for start in starts]
            return jnp.concatenate(taken, axis=0).reshape(part * breadth, channels)

        pieces = []
        for tap in range(3):
            beside = jnp.concatenate(
                [sides[i * slots + tap : i * slots + tap + count] for i in range(len(starts))], axis=0
            ).reshape(part * breadth, 2 * channels)
            pieces += [beside[:, :channels], rows_from(tap), beside[:, channels:]]
        total = jnp.dot(
            jnp.concatenate(pieces, axis=1), weight[...], preferred_element_type=jnp.float32
        ) + bias[...]
        result = rows_from(1).astype(jnp.float32) + jnp.maximum(total, 0.0)
        result = result.astype(jnp.bfloat16).reshape(part, breadth, channels)
        base = step * part

        @pl.when(image == LEFT)
        def _():
            enc[LEFT, pl.ds(base, part)] = result

            @pl.when(even & has_two & (step > 0))
            def _():
                back_copy(step).start()

        def turned(row):
            return jnp.dot(flip, result[row], preferred_element_type=jnp.float32).astype(jnp.bfloat16)

        @pl.when((image == AHEAD) & odd)
        def _():
            for row in range(part):
                far[base + row] = turned(row)
            pass_copy(step).start()

        @pl.when((image == AHEAD) & even)
        def _():
            back[pl.ds(base, part)] = result

        @pl.when(image == RIGHT)
        def _():
            for row in range(part):
                enc[RIGHT, base + row] = turned(row)

            @pl.when(even)
            def _():
                own_copy(step).start()

            @pl.when(odd & gives_two & (step > 0))
            def _():
                far_copy(step).start()

    def conv_inner(image, low, high):
        def body(step, carry):
            convolve(image, step, step // spans, [edge + lax.rem(step, spans) * part], part)
            return carry

        lax.fori_loop(low, high, body, 0)

    def conv_edge(image):
        def body(step, carry):
            convolve(image, step, step - inner, [0, height - edge], edge)
            return carry

        lax.fori_loop(inner, chunks, body, 0)

    def both(act, image):
        for choice in (RIGHT, LEFT):

            @pl.when(image == choice)
            def _():
                act(choice)

    def product(keys, queries):
        return lax.dot_general(
            keys, queries, (((1,), (1,)), ((), ())), preferred_element_type=jnp.float32
        )

    half_blocks = breadth // 16
    lane8 = lax.broadcasted_iota(jnp.int32, (8, breadth), 1)

    def triangle(step, carry):
        base = step * part

        @pl.when(step > 0)
        def _():
            back_copy(step).wait_recv()

        for pair in range(0, part, 2):
            two = [product(enc[RIGHT, base + row], back[base + row]) for row in (pair, pair + 1)]
            for i in range(half_blocks + 1):
                cut = breadth - 8 * i
                kept = []
                for block in two:
                    piece = block[8 * i : 8 * i + 8]
                    if 0 < i < half_blocks:
                        piece = jnp.where(lane8 < cut, piece, pltpu.roll(block[cut : cut + 8], cut, 1))
                    kept.append(piece)
                tri_out[(base + pair) // 2, i] = jnp.concatenate(kept, axis=0).astype(jnp.bfloat16)
        tri_copy(step).start()
        return carry

    def triangles(low, high):
        @pl.when(even & gives_two)
        def _():
            lax.fori_loop(low, high, triangle, 0)

    both(functools.partial(wait_halo, COL_SIDES), first)

    both(functools.partial(send_ahead, 1), first)
    conv_inner(first, 0, inner)
    both(functools.partial(wait_halo, COL_SIDES), second)
    both(functools.partial(send_ahead, 1), second)
    conv_inner(second, 0, inner)
    for choice, when in takes_ahead:

        @pl.when(when)
        def _():
            ahead_copy(0, choice).wait_recv()
            ahead_copy(1, choice).wait_recv()

    any_ahead = (odd & has_two) | (even & gives_two)
    conv_inner(AHEAD, 0, jnp.where(any_ahead, 1, 0))
    both(functools.partial(wait_halo, ROW_SIDES + CORNERS), first)
    conv_edge(first)
    triangles(0, inner)
    both(functools.partial(wait_halo, ROW_SIDES + CORNERS), second)
    conv_edge(second)
    triangles(inner, chunks)

    def finish(step, scores):
        base = step * part

        @pl.when(odd)
        def _():
            own_copy(step).wait_recv()

        @pl.when(odd & has_two)
        def _():
            @pl.when(step > 0)
            def _():
                far_copy(step).wait_recv()
                pass_copy(step).start()

            for row in range(part):
                scores[row, 2 * breadth : 3 * breadth] = product(
                    far[base + row], enc[LEFT, base + row]
                )

        @pl.when(even & has_two)
        def _():
            pass_copy(step).wait_recv()
            tri_copy(step).wait_recv()
            for pair in range(0, part, 2):
                for i in range(half_blocks + 1):
                    both_rows = tri_in[(base + pair) // 2, i].astype(jnp.float32)
                    for row in range(2):
                        block = both_rows[8 * row : 8 * row + 8]
                        start = 2 * breadth + 8 * i
                        scores[pair + row, start : start + 8] = block
                        if 0 < i < half_blocks:
                            start = 3 * breadth - 8 * i
                            scores[pair + row, start : start + 8] = pltpu.roll(block, 8 * i, 1)

        for row in range(part):
            scores[row, :breadth] = product(enc[RIGHT, base + row], enc[LEFT, base + row])
            scores[row, breadth : 2 * breadth] = product(near[base + row], enc[LEFT, base + row])
            if scores is not held:
                b, h = place_of(step, row)
                volume_row(
                    scores, stage, out, row, b * height + h, span_count, level_count, scale
                )

    def finish_one(step, carry):
        finish(step, scores)
        return carry

    lax.fori_loop(0, chunks - 1, finish_one, 0)

    @pl.when(even)
    def _():
        sent(enc.at[RIGHT], near, 0, 0, 1).wait_send()

    @pl.when(even & has_two)
    def _():
        sent(enc.at[LEFT], back, 1, part, -2).wait_send()

    @pl.when(odd & gives_two)
    def _():
        sent(enc.at[RIGHT], far, 0, part, 2).wait_send()

    for choice, when in sends_ahead:

        @pl.when(when)
        def _():
            ahead_copy(0, choice).wait_send()
            ahead_copy(1, choice).wait_send()

    for side in range(8):

        @pl.when(inside(*AROUND[side]))
        def _():
            halo_copy(side, pl.ds(0, 2)).wait_send()

    finish(chunks - 1, held)

    @pl.when(odd & has_two)
    def _():
        sent(far, near, 1, 0, -1).wait_send()

    @pl.when(even & gives_two)
    def _():
        sent(tri_out, tri_in, 2, 0, 2).wait_send()


def store_kernel(batch, height, part, span_count, level_count, scale, done, held, out, tail, stage, sems):
    edge = part // 2
    last = (batch - 1) * height
    pieces = [(b * height + h, part) for b in range(batch - 1) for h in range(0, height, part)]
    pieces += [(last + h, part) for h in range(edge, height - edge, part)]
    copies = []
    for start, size in pieces:
        rows = pl.ds(start, size)
        copies.append(pltpu.make_async_copy(done.at[rows], out.at[rows], sems.at[len(copies)]))
    for copy in copies:
        copy.start()
    for half, start in enumerate((last, last + height - edge)):
        for row in range(half * edge, half * edge + edge):
            volume_row(held, stage, tail, row, row, span_count, level_count, scale)
        copies.append(
            pltpu.make_async_copy(
                tail.at[pl.ds(half * edge, edge)], out.at[pl.ds(start, edge)], sems.at[len(copies)]
            )
        )
        copies[-1].start()
    for copy in copies:
        copy.wait()


def in_hbm(array):
    return pltpu.with_memory_space_constraint(array, pltpu.HBM)


def shards(left_features, right_features, conv_weight, conv_bias):
    batch, height, breadth, channels = left_features.shape
    col_count = lax.axis_size("cols")
    part = math.gcd(height, 4)
    assert 2 * breadth == DISP and col_count % 2 == 0 and breadth % 16 == 0
    assert part % 2 == 0 and height > part
    lines = batch * height
    chunks = lines // part
    width = sum(DISP >> level for level in range(LEVELS))
    hbm = pl.BlockSpec(memory_space=pltpu.HBM)
    vmem = pl.BlockSpec(memory_space=pltpu.VMEM)
    dma = pltpu.SemaphoreType.DMA
    bf16, f32 = jnp.bfloat16, jnp.float32
    tri = (lines // 2, breadth // 16 + 1, 16, breadth)
    stage = pltpu.VMEM((part, 3, DISP + 16, breadth), f32)
    scale = 1.0 / math.sqrt(channels)
    done, held = pl.pallas_call(
        functools.partial(
            kernel, lax.axis_size("rows"), col_count, part, DISP, LEVELS, scale
        ),
        out_shape=[
            jax.ShapeDtypeStruct((lines, width, breadth), f32),
            jax.ShapeDtypeStruct((part, 3 * breadth, breadth), f32),
        ],
        in_specs=[hbm] * 4,
        out_specs=[vmem] * 2,
        scratch_shapes=[
            pltpu.VMEM((3, batch, height + 2, breadth, channels), bf16),
            pltpu.VMEM((part + 4, breadth, 2 * channels), bf16),
            pltpu.VMEM((2, 2, batch, height, 16, channels), bf16),
            pltpu.VMEM((2, 2, batch, height, 1, channels), f32),
            pltpu.VMEM((2, 3, batch, height + 2, 1, channels), f32),
            pltpu.VMEM((9 * channels, channels), bf16),
            pltpu.VMEM((1, channels), f32),
            pltpu.VMEM((2, lines, breadth, channels), bf16),
            pltpu.VMEM((lines, breadth, channels), bf16),
            pltpu.VMEM((lines, breadth, channels), bf16),
            pltpu.VMEM((lines, breadth, channels), bf16),
            pltpu.VMEM(tri, bf16),
            pltpu.VMEM(tri, bf16),
            pltpu.VMEM((part, 3 * breadth, breadth), f32),
            stage,
            dma((4,)), dma((2, 2)), dma((8,)), dma((2, 8)), dma((2, 2)),
            dma((3,)), dma((chunks,)), dma((chunks,)), dma((chunks,)),
        ],
        compiler_params=pltpu.CompilerParams(
            collective_id=0, has_side_effects=True, vmem_limit_bytes=40 * 2**20
        ),
    )(
        in_hbm(left_features), in_hbm(right_features),
        in_hbm(conv_weight.reshape(9 * channels, channels)), in_hbm(conv_bias.reshape(1, -1)),
    )
    out = pl.pallas_call(
        functools.partial(store_kernel, batch, height, part, DISP, LEVELS, scale),
        out_shape=jax.ShapeDtypeStruct((lines, width, breadth), f32),
        in_specs=[vmem] * 2,
        out_specs=hbm,
        scratch_shapes=[
            pltpu.VMEM((part, width, breadth), f32), stage, dma((chunks + 1,)),
        ],
        compiler_params=pltpu.CompilerParams(vmem_limit_bytes=8 * 2**20),
    )(done, held)
    return jnp.swapaxes(out, 1, 2).reshape(batch, height, breadth, -1)


def solution(mesh):
    return jax.shard_map(
        shards,
        mesh=mesh,
        in_specs=(P(None, "rows", "cols", None), P(None, "rows", "cols", None), P(), P()),
        out_specs=P(None, "rows", "cols", None),
        check_vma=False,
    )
```

```python
import functools
import math

import jax
import jax.numpy as jnp
from jax import lax
from jax.experimental import pallas as pl
from jax.experimental.pallas import tpu as pltpu
from jax.sharding import PartitionSpec as P

DISP = 256
LEVELS = 4


MESH = pl.DeviceIdType.MESH
AROUND = ((-1, 0), (1, 0), (0, -1), (0, 1), (-1, -1), (-1, 1), (1, -1), (1, 1))
OPPOSITE = (1, 0, 3, 2, 7, 6, 5, 4)
ROW_SIDES = (0, 1)
COL_SIDES = (2, 3)
CORNERS = (4, 5, 6, 7)
LEFT, RIGHT = 0, 1
RIM = 16


def volume_row(scores, stage, out, slot, line, span_count, level_count, scale):
    breadth = scores.shape[2]
    steps = breadth - 1 - lax.broadcasted_iota(jnp.int32, (1, breadth), 1)
    bit = breadth // 2
    value = None
    while bit >= 8:
        keep = span_count + bit
        if value is None:
            low, high = scores[slot, :keep], scores[slot, bit : bit + keep]
        else:
            low, high = value[:keep], value[bit : bit + keep]
        value = jnp.where((steps & bit) != 0, high, low)
        bit //= 2
    for index, bit in enumerate((4, 2, 1)):
        keep = span_count + (8 if bit > 1 else 0)
        stage[slot, index, : span_count + 8] = value
        value = jnp.where((steps & bit) != 0, stage[slot, index, pl.ds(bit, keep)], value[:keep])
    out[line, :span_count] = value * scale
    start, size = 0, span_count
    for _ in range(1, level_count):
        half = size // 2
        pooled = (
            out[line, pl.ds(start, half, stride=2)] + out[line, pl.ds(start + 1, half, stride=2)]
        ) * 0.5
        start, size = start + size, half
        out[line, start : start + half] = pooled


def kernel(
    row_count, col_count, part, span_count, level_count, scale,
    left, right, weight_hbm, bias_hbm, out, held,
    images, sides, raw_edges, edges, col_halo, weight, bias, enc, early, near, far, back, tri_out, tri_in, scores, stage,
    in_sems, edge_sems, halo_sems, recv_sem, early_sems, rim_sems, send_sems, near_sems, two_sems, back_sems, go_sem,
):
    batch, height, breadth, channels = left.shape
    my_row, my_col = lax.axis_index("rows"), lax.axis_index("cols")
    edge = part // 2
    spans = height // part - 1
    chunks = batch * (spans + 1)
    inner = batch * spans
    ahead = min(inner, 2)

    def inside(step_row, step_col):
        row, col = my_row + step_row, my_col + step_col
        return (row >= 0) & (row < row_count) & (col >= 0) & (col < col_count)

    odd = lax.rem(my_col, 2) == 1
    even = jnp.logical_not(odd)
    has_two = my_col >= 2
    gives_two = my_col + 2 < col_count
    has_near = my_col >= 1
    first = jnp.where(gives_two, RIGHT, LEFT)
    second = 1 - first

    def fetch(image):
        source = right if image == RIGHT else left
        return pltpu.make_async_copy(
            source, images.at[image, :, pl.ds(1, height)], in_sems.at[image]
        )

    def fetch_edge(side, image):
        source = right if image == RIGHT else left
        return pltpu.make_async_copy(
            source.at[:, :, pl.ds(side * (breadth - 16), 16)],
            raw_edges.at[side, image], edge_sems.at[side, image],
        )

    def fetch_weight():
        return pltpu.make_async_copy(weight_hbm, weight, in_sems.at[2])

    def fetch_bias():
        return pltpu.make_async_copy(bias_hbm, bias, in_sems.at[3])

    barrier = pltpu.get_barrier_semaphore()
    partners = AROUND + ((0, -2), (0, 2))
    for step_row, step_col in partners:

        @pl.when(inside(step_row, step_col))
        def _():
            pl.semaphore_signal(
                barrier, inc=1, device_id=(my_row + step_row, my_col + step_col), device_id_type=MESH
            )

    for image in (RIGHT, LEFT):

        @pl.when(first == image)
        def _():
            for choice in (image, 1 - image):
                for side in range(2):
                    fetch_edge(side, choice).start()
            fetch(image).start()
            fetch_weight().start()
            fetch_bias().start()
            fetch(1 - image).start()

    def halo_copy(side, image):
        step_row, step_col = AROUND[side]
        if step_col == 0:
            source = images.at[image, :, 1 if step_row < 0 else height]
            target = images.at[image, :, height + 1 if step_row < 0 else 0]
        else:
            mine, theirs = (0, 1) if step_col < 0 else (1, 0)
            if step_row == 0:
                source = edges.at[mine, image]
                target = col_halo.at[theirs, image, :, pl.ds(1, height)]
            else:
                source = edges.at[mine, image, :, 0 if step_row < 0 else height - 1]
                target = col_halo.at[theirs, image, :, height + 1 if step_row < 0 else 0]
        return pltpu.make_async_remote_copy(
            src_ref=source, dst_ref=target,
            send_sem=halo_sems.at[side],
            recv_sem=recv_sem.at[image if isinstance(image, int) else 0, OPPOSITE[side]],
            device_id=(my_row + step_row, my_col + step_col), device_id_type=MESH,
        )

    sends_early = ((RIGHT, odd & gives_two), (LEFT, even & has_two))

    def take_edges(image):
        for b in range(batch):
            for h in range(height):
                edges[0, image, b, h] = raw_edges[0, image, b, h].astype(jnp.float32)[0:1]
                edges[1, image, b, h] = raw_edges[1, image, b, h].astype(jnp.float32)[15:16]

    def send_halo(which, image):
        for side in which:

            @pl.when(inside(*AROUND[side]))
            def _():
                halo_copy(side, image).start()

    def wait_halo(which, image):
        for side in which:

            @pl.when(inside(*AROUND[OPPOSITE[side]]))
            def _():
                halo_copy(side, image).wait_recv()

    def clear_halo():
        for side in range(8):
            step_row, step_col = AROUND[side]

            @pl.when(jnp.logical_not(inside(step_row, step_col)))
            def _():
                line = 0 if step_row < 0 else height + 1
                for image in (LEFT, RIGHT):
                    for b in range(batch):
                        if step_col == 0:
                            images[image, b, line] = jnp.zeros((breadth, channels), jnp.bfloat16)
                        elif step_row == 0:
                            col_halo[0 if step_col < 0 else 1, image, b, pl.ds(1, height)] = jnp.zeros(
                                (height, 1, channels), jnp.float32
                            )
                        else:
                            col_halo[0 if step_col < 0 else 1, image, b, line] = jnp.zeros(
                                (1, channels), jnp.float32
                            )

    for image in (RIGHT, LEFT):

        @pl.when(first == image)
        def _():
            for side in range(2):
                fetch_edge(side, image).wait()

    take_edges(first)
    peers = sum(inside(*step).astype(jnp.int32) for step in partners)
    pl.semaphore_wait(barrier, peers)
    for image in (RIGHT, LEFT):

        @pl.when(first == image)
        def _():
            send_halo(COL_SIDES + CORNERS, image)
            for side in range(2):
                fetch_edge(side, 1 - image).wait()

    take_edges(second)
    for image in (RIGHT, LEFT):

        @pl.when(first == image)
        def _():
            send_halo(COL_SIDES + CORNERS, 1 - image)
            fetch(image).wait()
            send_halo(ROW_SIDES, image)
            fetch(1 - image).wait()
            send_halo(ROW_SIDES, 1 - image)

    clear_halo()

    @pl.when(jnp.logical_not(has_near))
    def _():
        near[...] = jnp.zeros_like(near)

    @pl.when(jnp.logical_not(has_two))
    def _():
        for target in (scores, held):
            target[:, 2 * breadth :] = jnp.zeros((part, breadth, breadth), jnp.float32)

    fetch_weight().wait()
    fetch_bias().wait()

    column = lax.broadcasted_iota(jnp.int32, (breadth, 1), 0)
    flip = jnp.where(
        lax.broadcasted_iota(jnp.int32, (breadth, breadth), 0)
        + lax.broadcasted_iota(jnp.int32, (breadth, breadth), 1)
        == breadth - 1,
        1.0, 0.0,
    ).astype(jnp.bfloat16)

    def place_of(step, row):
        is_inner = step < inner
        b = jnp.where(is_inner, step // spans, step - inner)
        h = jnp.where(
            is_inner,
            edge + lax.rem(step, spans) * part + row,
            row if row < edge else height - part + row,
        )
        return b, h

    def remote(source, target, send, recv, step, away, rows=part):
        lines = pl.ds(step * rows, rows)
        return pltpu.make_async_remote_copy(
            src_ref=source.at[lines], dst_ref=target.at[lines],
            send_sem=send_sems.at[send], recv_sem=recv.at[step],
            device_id=(my_row, my_col + away), device_id_type=MESH,
        )

    def own_copy(step):
        return remote(enc.at[RIGHT], near, 0, near_sems, step, 1)

    def far_copy(step):
        return remote(enc.at[RIGHT], far, jnp.where(step == chunks - 1, 3, 0), two_sems, step, 2)

    def pass_copy(step):
        return remote(far, near, 1, near_sems, step, -1)

    def back_copy(step):
        return remote(enc.at[LEFT], back, 1, back_sems, step, -2)

    def tri_copy(step):
        return remote(tri_out, tri_in, 2, two_sems, step, 2, 1)

    def toward_two(image):
        return (far, my_col + 2) if image == RIGHT else (back, my_col - 2)

    def early_copy(piece, image):
        target, col = toward_two(image)
        lines, pixels = pl.ds(piece * edge, edge), pl.ds(RIM, breadth - 2 * RIM)
        return pltpu.make_async_remote_copy(
            src_ref=early.at[lines, pixels], dst_ref=target.at[lines, pixels],
            send_sem=send_sems.at[4], recv_sem=early_sems.at[piece],
            device_id=(my_row, col), device_id_type=MESH,
        )

    def rim_copy(step, side, image):
        target, col = toward_two(image)
        lines, pixels = pl.ds(step * part, part), pl.ds(side * (breadth - RIM), RIM)
        return pltpu.make_async_remote_copy(
            src_ref=enc.at[image, lines, pixels], dst_ref=target.at[lines, pixels],
            send_sem=send_sems.at[5], recv_sem=rim_sems.at[2 * step + side],
            device_id=(my_row, col), device_id_type=MESH,
        )

    def wait_two(step, image):
        @pl.when(step < ahead)
        def _():
            for half in range(2):
                early_copy(2 * step + half, image).wait_recv()
                rim_copy(step, half, image).wait_recv()

        @pl.when(step >= ahead)
        def _():
            (far_copy if image == RIGHT else back_copy)(step).wait_recv()

    def start_two(step, image):
        @pl.when(step < ahead)
        def _():
            for side in range(2):
                rim_copy(step, side, image).start()

        @pl.when(step >= ahead)
        def _():
            (far_copy if image == RIGHT else back_copy)(step).start()

    def sent_early(image):
        target, col = toward_two(image)
        lines = pl.ds(0, ahead * part)
        for send, source, pixels in (
            (4, early, pl.ds(RIM, breadth - 2 * RIM)), (5, enc.at[image], pl.ds(0, 2 * RIM))
        ):
            yield pltpu.make_async_remote_copy(
                src_ref=source.at[lines, pixels], dst_ref=target.at[lines, pixels],
                send_sem=send_sems.at[send], recv_sem=near_sems.at[0],
                device_id=(my_row, col), device_id_type=MESH,
            )

    def sent(source, target, send, away, low=0, high=chunks, rows=part):
        lines = pl.ds(low * rows, (high - low) * rows)
        return pltpu.make_async_remote_copy(
            src_ref=source.at[lines], dst_ref=target.at[lines],
            send_sem=send_sems.at[send], recv_sem=near_sems.at[0],
            device_id=(my_row, my_col + away), device_id_type=MESH,
        )

    def encoded(image, b, starts, count, bare):
        slots = count + 2
        rows = count * len(starts)
        for piece, start in enumerate(starts):
            for line in range(slots):
                row = images[image, b, start + line].astype(jnp.float32)
                before = 0.0 if bare else col_halo[0, image, b, start + line]
                after = 0.0 if bare else col_halo[1, image, b, start + line]
                sides[piece * slots + line, :, :channels] = jnp.where(
                    column == 0, before, pltpu.roll(row, 1, 0)
                ).astype(jnp.bfloat16)
                sides[piece * slots + line, :, channels:] = jnp.where(
                    column == breadth - 1, after, pltpu.roll(row, breadth - 1, 0)
                ).astype(jnp.bfloat16)

        def rows_from(offset):
            taken = [images[image, b, pl.ds(start + offset, count)] for start in starts]
            return jnp.concatenate(taken, axis=0).reshape(rows * breadth, channels)

        pieces = []
        for tap in range(3):
            beside = jnp.concatenate(
                [sides[i * slots + tap : i * slots + tap + count] for i in range(len(starts))], axis=0
            ).reshape(rows * breadth, 2 * channels)
            pieces += [beside[:, :channels], rows_from(tap), beside[:, channels:]]
        total = jnp.dot(
            jnp.concatenate(pieces, axis=1), weight[...], preferred_element_type=jnp.float32
        ) + bias[...]
        result = rows_from(1).astype(jnp.float32) + jnp.maximum(total, 0.0)
        return result.astype(jnp.bfloat16).reshape(rows, breadth, channels)

    def turned(plain):
        return jnp.dot(flip, plain, preferred_element_type=jnp.float32).astype(jnp.bfloat16)

    def convolve(image, step, b, starts, count):
        result = encoded(image, b, starts, count, False)
        base = step * part

        @pl.when(image == LEFT)
        def _():
            enc[LEFT, pl.ds(base, part)] = result

            @pl.when(even & has_two)
            def _():
                start_two(step, LEFT)

        @pl.when(image == RIGHT)
        def _():
            for row in range(part):
                enc[RIGHT, base + row] = turned(result[row])

            @pl.when(even)
            def _():
                own_copy(step).start()

            @pl.when(odd & gives_two)
            def _():
                start_two(step, RIGHT)

    def conv_early(piece, carry):
        step = piece // 2
        start = edge + lax.rem(step, spans) * part + lax.rem(piece, 2) * edge
        image = jnp.where(odd, RIGHT, LEFT)
        result = encoded(image, step // spans, [start], edge, True)

        @pl.when(odd)
        def _():
            for row in range(edge):
                early[piece * edge + row] = turned(result[row])
            early_copy(piece, RIGHT).start()

        @pl.when(even)
        def _():
            early[pl.ds(piece * edge, edge)] = result
            early_copy(piece, LEFT).start()

        return carry

    def conv_inner(image):
        def body(step, carry):
            convolve(image, step, step // spans, [edge + lax.rem(step, spans) * part], part)
            return carry

        lax.fori_loop(0, inner, body, 0)

    def conv_edge(image):
        def body(step, carry):
            convolve(image, step, step - inner, [0, height - edge], edge)
            return carry

        lax.fori_loop(inner, chunks, body, 0)

    def both(act, image):
        for choice in (RIGHT, LEFT):

            @pl.when(image == choice)
            def _():
                act(choice)

    def product(keys, queries):
        return lax.dot_general(
            keys, queries, (((1,), (1,)), ((), ())), preferred_element_type=jnp.float32
        )

    half_blocks = breadth // 16
    lane8 = lax.broadcasted_iota(jnp.int32, (8, breadth), 1)

    def triangle(step, carry):
        base = step * part
        wait_two(step, LEFT)
        packed, middles = [], []
        for row in range(part):
            block = product(enc[RIGHT, base + row], back[base + row])
            packed.append(block[0:8])
            for i in range(1, half_blocks):
                cut = breadth - 8 * i
                packed.append(
                    jnp.where(
                        lane8 < cut, block[8 * i : 8 * i + 8], pltpu.roll(block[cut : cut + 8], cut, 1)
                    )
                )
            middles.append(block[8 * half_blocks : 8 * half_blocks + 8])
        for row in range(0, part, 2):
            packed.append(
                jnp.where(
                    lane8 < breadth // 2, middles[row], pltpu.roll(middles[row + 1], breadth // 2, 1)
                )
            )
        packed += packed[: len(packed) % 2]
        for i in range(len(packed) // 2):
            tile = jnp.concatenate(packed[2 * i : 2 * i + 2], axis=0)
            tri_out[step, i] = tile.astype(jnp.bfloat16)

        @pl.when(step >= inner)
        def _():
            tri_copy(step).start()

        return carry

    def unpack_triangle(step, scores):
        def packed(index):
            tile = tri_in[step, index // 2].astype(jnp.float32)
            return tile[8 * (index % 2) : 8 * (index % 2) + 8]

        def put(row, block_row, block):
            start = 2 * breadth + 8 * block_row
            scores[row, start : start + 8] = block

        for row in range(part):
            for i in range(half_blocks):
                block = packed(row * half_blocks + i)
                put(row, i, block)
                if i > 0:
                    put(row, 2 * half_blocks - i, pltpu.roll(block, 8 * i, 1))
            block = packed(part * half_blocks + row // 2)
            put(row, half_blocks, block if row % 2 == 0 else pltpu.roll(block, breadth // 2, 1))

    def send_triangle(step, carry):
        tri_copy(step).start()
        return carry

    def triangles(low, high):
        @pl.when(even & gives_two)
        def _():
            lax.fori_loop(low, high, triangle, 0)

    @pl.when((odd & gives_two) | (even & has_two))
    def _():
        lax.fori_loop(0, 2 * ahead, conv_early, 0)

    both(functools.partial(wait_halo, COL_SIDES), first)
    conv_inner(first)
    both(functools.partial(wait_halo, COL_SIDES), second)
    conv_inner(second)
    both(functools.partial(wait_halo, ROW_SIDES + CORNERS), first)
    conv_edge(first)
    triangles(0, inner)
    both(functools.partial(wait_halo, ROW_SIDES + CORNERS), second)
    conv_edge(second)

    @pl.when(even & gives_two)
    def _():
        pl.semaphore_wait(go_sem, 1)
        lax.fori_loop(0, inner, send_triangle, 0)

    triangles(inner, chunks)


    def finish(step, scores):
        base = step * part

        @pl.when(odd)
        def _():
            own_copy(step).wait_recv()

        @pl.when(odd & has_two)
        def _():
            wait_two(step, RIGHT)
            pass_copy(step).start()
            for row in range(part):
                scores[row, 2 * breadth : 3 * breadth] = product(
                    far[base + row], enc[LEFT, base + row]
                )

        @pl.when(even & has_two)
        def _():
            pass_copy(step).wait_recv()

        def take_triangle():
            @pl.when(even & has_two)
            def _():
                tri_copy(step).wait_recv()
                unpack_triangle(step, scores)

        if scores is not held:
            take_triangle()
        for row in range(part):
            scores[row, :breadth] = product(enc[RIGHT, base + row], enc[LEFT, base + row])
            scores[row, breadth : 2 * breadth] = product(near[base + row], enc[LEFT, base + row])
            if scores is not held:
                b, h = place_of(step, row)
                volume_row(
                    scores, stage, out, row, b * height + h, span_count, level_count, scale
                )
        if scores is held:
            take_triangle()

    def finish_one(step, carry):
        finish(step, scores)
        return carry

    lax.fori_loop(0, chunks - 1, finish_one, 0)

    @pl.when(odd & gives_two)
    def _():
        sent(enc.at[RIGHT], far, 0, 2, ahead, chunks - 1).wait_send()
        pl.semaphore_signal(go_sem, inc=1, device_id=(my_row, my_col - 1), device_id_type=MESH)

    @pl.when(even)
    def _():
        sent(enc.at[RIGHT], near, 0, 1).wait_send()

    @pl.when(even & has_two)
    def _():
        sent(enc.at[LEFT], back, 1, -2, ahead).wait_send()

    for choice, when in sends_early:

        @pl.when(when)
        def _():
            for copy in sent_early(choice):
                copy.wait_send()

    for side in range(8):

        @pl.when(inside(*AROUND[side]))
        def _():
            halo_copy(side, pl.ds(0, 2)).wait_send()

    finish(chunks - 1, held)

    @pl.when(odd & has_two)
    def _():
        sent(far, near, 1, -1).wait_send()

    @pl.when(even & gives_two)
    def _():
        sent(tri_out, tri_in, 2, 2, rows=1).wait_send()

    @pl.when(odd & gives_two)
    def _():
        sent(enc.at[RIGHT], far, 3, 2, chunks - 1).wait_send()


def store_kernel(batch, height, part, span_count, level_count, scale, done, held, out, tail, stage, sems):
    edge = part // 2
    last = (batch - 1) * height
    pieces = [(b * height + h, part) for b in range(batch - 1) for h in range(0, height, part)]
    pieces += [(last + h, part) for h in range(edge, height - edge, part)]
    copies = []
    for start, size in pieces:
        rows = pl.ds(start, size)
        copies.append(pltpu.make_async_copy(done.at[rows], out.at[rows], sems.at[len(copies)]))
    for copy in copies:
        copy.start()
    for half, start in enumerate((last, last + height - edge)):
        for row in range(half * edge, half * edge + edge):
            volume_row(held, stage, tail, row, row, span_count, level_count, scale)
        copies.append(
            pltpu.make_async_copy(
                tail.at[pl.ds(half * edge, edge)], out.at[pl.ds(start, edge)], sems.at[len(copies)]
            )
        )
        copies[-1].start()
    for copy in copies:
        copy.wait()


def in_hbm(array):
    return pltpu.with_memory_space_constraint(array, pltpu.HBM)


def shards(left_features, right_features, conv_weight, conv_bias):
    batch, height, breadth, channels = left_features.shape
    col_count = lax.axis_size("cols")
    part = math.gcd(height, 4)
    assert 2 * breadth == DISP and col_count % 2 == 0 and breadth % 32 == 0
    assert part % 2 == 0 and height > part
    lines = batch * height
    chunks = lines // part
    ahead = min(chunks - batch, 2)
    width = sum(DISP >> level for level in range(LEVELS))
    hbm = pl.BlockSpec(memory_space=pltpu.HBM)
    vmem = pl.BlockSpec(memory_space=pltpu.VMEM)
    dma = pltpu.SemaphoreType.DMA
    bf16, f32 = jnp.bfloat16, jnp.float32
    tri = (chunks, pl.cdiv(part * (breadth // 16) + part // 2, 2), 16, breadth)
    stage = pltpu.VMEM((part, 3, DISP + 16, breadth), f32)
    scale = 1.0 / math.sqrt(channels)
    done, held = pl.pallas_call(
        functools.partial(
            kernel, lax.axis_size("rows"), col_count, part, DISP, LEVELS, scale
        ),
        out_shape=[
            jax.ShapeDtypeStruct((lines, width, breadth), f32),
            jax.ShapeDtypeStruct((part, 3 * breadth, breadth), f32),
        ],
        in_specs=[hbm] * 4,
        out_specs=[vmem] * 2,
        scratch_shapes=[
            pltpu.VMEM((2, batch, height + 2, breadth, channels), bf16),
            pltpu.VMEM((part + 4, breadth, 2 * channels), bf16),
            pltpu.VMEM((2, 2, batch, height, 16, channels), bf16),
            pltpu.VMEM((2, 2, batch, height, 1, channels), f32),
            pltpu.VMEM((2, 2, batch, height + 2, 1, channels), f32),
            pltpu.VMEM((9 * channels, channels), bf16),
            pltpu.VMEM((1, channels), f32),
            pltpu.VMEM((2, lines, breadth, channels), bf16),
            pltpu.VMEM((ahead * part, breadth, channels), bf16),
            pltpu.VMEM((lines, breadth, channels), bf16),
            pltpu.VMEM((lines, breadth, channels), bf16),
            pltpu.VMEM((lines, breadth, channels), bf16),
            pltpu.VMEM(tri, bf16),
            pltpu.VMEM(tri, bf16),
            pltpu.VMEM((part, 3 * breadth, breadth), f32),
            stage,
            dma((4,)), dma((2, 2)), dma((8,)), dma((2, 8)), dma((2 * ahead,)), dma((2 * ahead,)),
            dma((6,)), dma((chunks,)), dma((chunks,)), dma((chunks,)), pltpu.SemaphoreType.REGULAR,
        ],
        compiler_params=pltpu.CompilerParams(
            collective_id=0, has_side_effects=True, vmem_limit_bytes=40 * 2**20
        ),
    )(
        in_hbm(left_features), in_hbm(right_features),
        in_hbm(conv_weight.reshape(9 * channels, channels)), in_hbm(conv_bias.reshape(1, -1)),
    )
    out = pl.pallas_call(
        functools.partial(store_kernel, batch, height, part, DISP, LEVELS, scale),
        out_shape=jax.ShapeDtypeStruct((lines, width, breadth), f32),
        in_specs=[vmem] * 2,
        out_specs=hbm,
        scratch_shapes=[
            pltpu.VMEM((part, width, breadth), f32), stage, dma((chunks + 1,)),
        ],
        compiler_params=pltpu.CompilerParams(vmem_limit_bytes=8 * 2**20),
    )(done, held)
    return jnp.swapaxes(out, 1, 2).reshape(batch, height, breadth, -1)


def solution(mesh):
    return jax.shard_map(
        shards,
        mesh=mesh,
        in_specs=(P(None, "rows", "cols", None), P(None, "rows", "cols", None), P(), P()),
        out_specs=P(None, "rows", "cols", None),
        check_vma=False,
    )
```

```python
import functools
import math

import jax
import jax.numpy as jnp
from jax import lax
from jax.experimental import pallas as pl
from jax.experimental.pallas import tpu as pltpu
from jax.sharding import PartitionSpec as P

DISP = 256
LEVELS = 4


MESH = pl.DeviceIdType.MESH
AROUND = ((-1, 0), (1, 0), (0, -1), (0, 1), (-1, -1), (-1, 1), (1, -1), (1, 1))
OPPOSITE = (1, 0, 3, 2, 7, 6, 5, 4)
ROW_SIDES = (0, 1)
COL_SIDES = (2, 3)
CORNERS = (4, 5, 6, 7)
LEFT, RIGHT = 0, 1
RIM = 16


def volume_row(scores, stage, out, slot, line, span_count, level_count, scale):
    breadth = scores.shape[2]
    steps = breadth - 1 - lax.broadcasted_iota(jnp.int32, (1, breadth), 1)
    bit = breadth // 2
    value = None
    while bit >= 8:
        keep = span_count + bit
        if value is None:
            low, high = scores[slot, :keep], scores[slot, bit : bit + keep]
        else:
            low, high = value[:keep], value[bit : bit + keep]
        value = jnp.where((steps & bit) != 0, high, low)
        bit //= 2
    for index, bit in enumerate((4, 2, 1)):
        keep = span_count + (8 if bit > 1 else 0)
        stage[slot, index, : span_count + 8] = value
        value = jnp.where((steps & bit) != 0, stage[slot, index, pl.ds(bit, keep)], value[:keep])
    out[line, :span_count] = value * scale
    start, size = 0, span_count
    for _ in range(1, level_count):
        half = size // 2
        pooled = (
            out[line, pl.ds(start, half, stride=2)] + out[line, pl.ds(start + 1, half, stride=2)]
        ) * 0.5
        start, size = start + size, half
        out[line, start : start + half] = pooled


def kernel(
    row_count, col_count, part, span_count, level_count, scale,
    left, right, weight_hbm, bias_hbm, out, held,
    images, sides, raw_edges, edges, col_halo, weight, bias, enc, early, near, far, back, tri_out, tri_in, scores, stage,
    in_sems, edge_sems, halo_sems, recv_sem, early_sems, rim_sems, send_sems, near_sems, two_sems, back_sems, go_sem,
):
    batch, height, breadth, channels = left.shape
    my_row, my_col = lax.axis_index("rows"), lax.axis_index("cols")
    edge = part // 2
    spans = height // part - 1
    chunks = batch * (spans + 1)
    inner = batch * spans
    ahead = min(inner, 2)

    def inside(step_row, step_col):
        row, col = my_row + step_row, my_col + step_col
        return (row >= 0) & (row < row_count) & (col >= 0) & (col < col_count)

    odd = lax.rem(my_col, 2) == 1
    even = jnp.logical_not(odd)
    has_two = my_col >= 2
    gives_two = my_col + 2 < col_count
    has_near = my_col >= 1
    first = jnp.where(gives_two, RIGHT, LEFT)
    second = 1 - first

    def fetch(image):
        source = right if image == RIGHT else left
        return pltpu.make_async_copy(
            source, images.at[image, :, pl.ds(1, height)], in_sems.at[image]
        )

    def fetch_edge(side, image):
        source = right if image == RIGHT else left
        return pltpu.make_async_copy(
            source.at[:, :, pl.ds(side * (breadth - 16), 16)],
            raw_edges.at[side, image], edge_sems.at[side, image],
        )

    def fetch_weight():
        return pltpu.make_async_copy(weight_hbm, weight, in_sems.at[2])

    def fetch_bias():
        return pltpu.make_async_copy(bias_hbm, bias, in_sems.at[3])

    barrier = pltpu.get_barrier_semaphore()
    partners = AROUND + ((0, -2), (0, 2))
    for step_row, step_col in partners:

        @pl.when(inside(step_row, step_col))
        def _():
            pl.semaphore_signal(
                barrier, inc=1, device_id=(my_row + step_row, my_col + step_col), device_id_type=MESH
            )

    for image in (RIGHT, LEFT):

        @pl.when(first == image)
        def _():
            for choice in (image, 1 - image):
                for side in range(2):
                    fetch_edge(side, choice).start()
            fetch(image).start()
            fetch_weight().start()
            fetch_bias().start()
            fetch(1 - image).start()

    def halo_copy(side, image):
        step_row, step_col = AROUND[side]
        if step_col == 0:
            source = images.at[image, :, 1 if step_row < 0 else height]
            target = images.at[image, :, height + 1 if step_row < 0 else 0]
        else:
            mine, theirs = (0, 1) if step_col < 0 else (1, 0)
            if step_row == 0:
                source = edges.at[mine, image]
                target = col_halo.at[theirs, image, :, pl.ds(1, height)]
            else:
                source = edges.at[mine, image, :, 0 if step_row < 0 else height - 1]
                target = col_halo.at[theirs, image, :, height + 1 if step_row < 0 else 0]
        return pltpu.make_async_remote_copy(
            src_ref=source, dst_ref=target,
            send_sem=halo_sems.at[side],
            recv_sem=recv_sem.at[image if isinstance(image, int) else 0, OPPOSITE[side]],
            device_id=(my_row + step_row, my_col + step_col), device_id_type=MESH,
        )

    sends_early = ((RIGHT, odd & gives_two), (LEFT, even & has_two))

    def take_edges(image):
        for b in range(batch):
            for h in range(height):
                edges[0, image, b, h] = raw_edges[0, image, b, h].astype(jnp.float32)[0:1]
                edges[1, image, b, h] = raw_edges[1, image, b, h].astype(jnp.float32)[15:16]

    def send_halo(which, image):
        for side in which:

            @pl.when(inside(*AROUND[side]))
            def _():
                halo_copy(side, image).start()

    def wait_halo(which, image):
        for side in which:

            @pl.when(inside(*AROUND[OPPOSITE[side]]))
            def _():
                halo_copy(side, image).wait_recv()

    def clear_halo():
        for side in range(8):
            step_row, step_col = AROUND[side]

            @pl.when(jnp.logical_not(inside(step_row, step_col)))
            def _():
                line = 0 if step_row < 0 else height + 1
                for image in (LEFT, RIGHT):
                    for b in range(batch):
                        if step_col == 0:
                            images[image, b, line] = jnp.zeros((breadth, channels), jnp.bfloat16)
                        elif step_row == 0:
                            col_halo[0 if step_col < 0 else 1, image, b, pl.ds(1, height)] = jnp.zeros(
                                (height, 1, channels), jnp.float32
                            )
                        else:
                            col_halo[0 if step_col < 0 else 1, image, b, line] = jnp.zeros(
                                (1, channels), jnp.float32
                            )

    for image in (RIGHT, LEFT):

        @pl.when(first == image)
        def _():
            for side in range(2):
                fetch_edge(side, image).wait()

    take_edges(first)
    peers = sum(inside(*step).astype(jnp.int32) for step in partners)
    pl.semaphore_wait(barrier, peers)
    for image in (RIGHT, LEFT):

        @pl.when(first == image)
        def _():
            send_halo(COL_SIDES + CORNERS, image)
            for side in range(2):
                fetch_edge(side, 1 - image).wait()

    take_edges(second)
    for image in (RIGHT, LEFT):

        @pl.when(first == image)
        def _():
            send_halo(COL_SIDES + CORNERS, 1 - image)
            fetch(image).wait()
            send_halo(ROW_SIDES, image)
            fetch(1 - image).wait()
            send_halo(ROW_SIDES, 1 - image)

    clear_halo()

    @pl.when(jnp.logical_not(has_near))
    def _():
        near[...] = jnp.zeros_like(near)

    @pl.when(jnp.logical_not(has_two))
    def _():
        for target in (scores, held):
            target[:, 2 * breadth :] = jnp.zeros((part, breadth, breadth), jnp.float32)

    fetch_weight().wait()
    fetch_bias().wait()

    column = lax.broadcasted_iota(jnp.int32, (breadth, 1), 0)
    flip = jnp.where(
        lax.broadcasted_iota(jnp.int32, (breadth, breadth), 0)
        + lax.broadcasted_iota(jnp.int32, (breadth, breadth), 1)
        == breadth - 1,
        1.0, 0.0,
    ).astype(jnp.bfloat16)

    def place_of(step, row):
        is_inner = step < inner
        b = jnp.where(is_inner, step // spans, step - inner)
        h = jnp.where(
            is_inner,
            edge + lax.rem(step, spans) * part + row,
            row if row < edge else height - part + row,
        )
        return b, h

    def remote(source, target, send, recv, step, away, rows=part):
        lines = pl.ds(step * rows, rows)
        return pltpu.make_async_remote_copy(
            src_ref=source.at[lines], dst_ref=target.at[lines],
            send_sem=send_sems.at[send], recv_sem=recv.at[step],
            device_id=(my_row, my_col + away), device_id_type=MESH,
        )

    def own_copy(step):
        return remote(enc.at[RIGHT], near, 0, near_sems, step, 1)

    def far_copy(step):
        return remote(enc.at[RIGHT], far, 0, two_sems, step, 2)

    def pass_copy(step):
        return remote(far, near, 1, near_sems, step, -1)

    def back_copy(step):
        return remote(enc.at[LEFT], back, 1, back_sems, step, -2)

    def tri_copy(step):
        return remote(tri_out, tri_in, 2, two_sems, step, 2, 1)

    def toward_two(image):
        return (far, my_col + 2) if image == RIGHT else (back, my_col - 2)

    def early_copy(piece, image):
        target, col = toward_two(image)
        lines, pixels = pl.ds(piece * edge, edge), pl.ds(RIM, breadth - 2 * RIM)
        return pltpu.make_async_remote_copy(
            src_ref=early.at[lines, pixels], dst_ref=target.at[lines, pixels],
            send_sem=send_sems.at[3], recv_sem=early_sems.at[piece // 2],
            device_id=(my_row, col), device_id_type=MESH,
        )

    def rim_copy(step, side, image):
        target, col = toward_two(image)
        lines, pixels = pl.ds(step * part, part), pl.ds(side * (breadth - RIM), RIM)
        return pltpu.make_async_remote_copy(
            src_ref=enc.at[image, lines, pixels], dst_ref=target.at[lines, pixels],
            send_sem=send_sems.at[4], recv_sem=rim_sems.at[step],
            device_id=(my_row, col), device_id_type=MESH,
        )

    def wait_two(step, image):
        @pl.when(step < ahead)
        def _():
            for copy in arrived_early(step, image):
                copy.wait_recv()

        @pl.when(step >= ahead)
        def _():
            (far_copy if image == RIGHT else back_copy)(step).wait_recv()

    def start_two(step, image):
        @pl.when(step < ahead)
        def _():
            for side in range(2):
                rim_copy(step, side, image).start()

        @pl.when(step >= ahead)
        def _():
            (far_copy if image == RIGHT else back_copy)(step).start()

    def pieces_of(first_step, steps, image):
        target, col = toward_two(image)
        lines = pl.ds(first_step * part, steps * part)
        for send, recv, source, pixels in (
            (3, early_sems, early, pl.ds(RIM, breadth - 2 * RIM)),
            (4, rim_sems, enc.at[image], pl.ds(0, 2 * RIM)),
        ):
            yield pltpu.make_async_remote_copy(
                src_ref=source.at[lines, pixels], dst_ref=target.at[lines, pixels],
                send_sem=send_sems.at[send], recv_sem=recv.at[first_step],
                device_id=(my_row, col), device_id_type=MESH,
            )

    def arrived_early(step, image):
        return pieces_of(jnp.minimum(step, ahead - 1), 1, image)

    def sent_early(image):
        return pieces_of(0, ahead, image)

    def sent(source, target, send, away, low=0, high=chunks, rows=part):
        lines = pl.ds(low * rows, (high - low) * rows)
        return pltpu.make_async_remote_copy(
            src_ref=source.at[lines], dst_ref=target.at[lines],
            send_sem=send_sems.at[send], recv_sem=near_sems.at[0],
            device_id=(my_row, my_col + away), device_id_type=MESH,
        )

    def encoded(image, b, starts, count, bare):
        slots = count + 2
        rows = count * len(starts)
        for piece, start in enumerate(starts):
            for line in range(slots):
                row = images[image, b, start + line].astype(jnp.float32)
                before = 0.0 if bare else col_halo[0, image, b, start + line]
                after = 0.0 if bare else col_halo[1, image, b, start + line]
                sides[piece * slots + line, :, :channels] = jnp.where(
                    column == 0, before, pltpu.roll(row, 1, 0)
                ).astype(jnp.bfloat16)
                sides[piece * slots + line, :, channels:] = jnp.where(
                    column == breadth - 1, after, pltpu.roll(row, breadth - 1, 0)
                ).astype(jnp.bfloat16)

        def rows_from(offset):
            taken = [images[image, b, pl.ds(start + offset, count)] for start in starts]
            return jnp.concatenate(taken, axis=0).reshape(rows * breadth, channels)

        pieces = []
        for tap in range(3):
            beside = jnp.concatenate(
                [sides[i * slots + tap : i * slots + tap + count] for i in range(len(starts))], axis=0
            ).reshape(rows * breadth, 2 * channels)
            pieces += [beside[:, :channels], rows_from(tap), beside[:, channels:]]
        total = jnp.dot(
            jnp.concatenate(pieces, axis=1), weight[...], preferred_element_type=jnp.float32
        ) + bias[...]
        result = rows_from(1).astype(jnp.float32) + jnp.maximum(total, 0.0)
        return result.astype(jnp.bfloat16).reshape(rows, breadth, channels)

    def turned(plain):
        return jnp.dot(flip, plain, preferred_element_type=jnp.float32).astype(jnp.bfloat16)

    def convolve(image, step, b, starts, count):
        result = encoded(image, b, starts, count, False)
        base = step * part

        @pl.when(image == LEFT)
        def _():
            enc[LEFT, pl.ds(base, part)] = result

            @pl.when(even & has_two)
            def _():
                start_two(step, LEFT)

        @pl.when(image == RIGHT)
        def _():
            for row in range(part):
                enc[RIGHT, base + row] = turned(result[row])

            @pl.when(even)
            def _():
                own_copy(step).start()

            @pl.when(odd & gives_two)
            def _():
                start_two(step, RIGHT)

    def conv_early(piece, carry):
        step = piece // 2
        start = edge + lax.rem(step, spans) * part + lax.rem(piece, 2) * edge
        image = jnp.where(odd, RIGHT, LEFT)
        result = encoded(image, step // spans, [start], edge, True)

        @pl.when(odd)
        def _():
            for row in range(edge):
                early[piece * edge + row] = turned(result[row])
            early_copy(piece, RIGHT).start()

        @pl.when(even)
        def _():
            early[pl.ds(piece * edge, edge)] = result
            early_copy(piece, LEFT).start()

        return carry

    def conv_inner(image):
        def body(step, carry):
            convolve(image, step, step // spans, [edge + lax.rem(step, spans) * part], part)
            return carry

        lax.fori_loop(0, inner, body, 0)

    def conv_edge(image):
        def body(step, carry):
            convolve(image, step, step - inner, [0, height - edge], edge)
            return carry

        lax.fori_loop(inner, chunks, body, 0)

    def both(act, image):
        for choice in (RIGHT, LEFT):

            @pl.when(image == choice)
            def _():
                act(choice)

    def product(keys, queries):
        return lax.dot_general(
            keys, queries, (((1,), (1,)), ((), ())), preferred_element_type=jnp.float32
        )

    half_blocks = breadth // 16
    lane8 = lax.broadcasted_iota(jnp.int32, (8, breadth), 1)

    def triangle(step, carry):
        base = step * part
        wait_two(step, LEFT)
        packed, middles = [], []
        for row in range(part):
            block = product(enc[RIGHT, base + row], back[base + row])
            packed.append(block[0:8])
            for i in range(1, half_blocks):
                cut = breadth - 8 * i
                packed.append(
                    jnp.where(
                        lane8 < cut, block[8 * i : 8 * i + 8], pltpu.roll(block[cut : cut + 8], cut, 1)
                    )
                )
            middles.append(block[8 * half_blocks : 8 * half_blocks + 8])
        for row in range(0, part, 2):
            packed.append(
                jnp.where(
                    lane8 < breadth // 2, middles[row], pltpu.roll(middles[row + 1], breadth // 2, 1)
                )
            )
        packed += packed[: len(packed) % 2]
        for i in range(len(packed) // 2):
            tile = jnp.concatenate(packed[2 * i : 2 * i + 2], axis=0)
            tri_out[step, i] = tile.astype(jnp.bfloat16)

        @pl.when(step >= inner)
        def _():
            tri_copy(step).start()

        return carry

    def unpack_triangle(step, scores):
        def packed(index):
            tile = tri_in[step, index // 2].astype(jnp.float32)
            return tile[8 * (index % 2) : 8 * (index % 2) + 8]

        def put(row, block_row, block):
            start = 2 * breadth + 8 * block_row
            scores[row, start : start + 8] = block

        for row in range(part):
            for i in range(half_blocks):
                block = packed(row * half_blocks + i)
                put(row, i, block)
                if i > 0:
                    put(row, 2 * half_blocks - i, pltpu.roll(block, 8 * i, 1))
            block = packed(part * half_blocks + row // 2)
            put(row, half_blocks, block if row % 2 == 0 else pltpu.roll(block, breadth // 2, 1))

    def send_triangle(step, carry):
        tri_copy(step).start()
        return carry

    def triangles(low, high):
        @pl.when(even & gives_two)
        def _():
            lax.fori_loop(low, high, triangle, 0)

    @pl.when((odd & gives_two) | (even & has_two))
    def _():
        lax.fori_loop(0, 2 * ahead, conv_early, 0)

    both(functools.partial(wait_halo, COL_SIDES), first)
    conv_inner(first)
    both(functools.partial(wait_halo, COL_SIDES), second)
    conv_inner(second)
    both(functools.partial(wait_halo, ROW_SIDES + CORNERS), first)
    conv_edge(first)
    triangles(0, inner)
    both(functools.partial(wait_halo, ROW_SIDES + CORNERS), second)
    conv_edge(second)

    @pl.when(odd & gives_two)
    def _():
        pl.semaphore_signal(go_sem, inc=1, device_id=(my_row, my_col - 1), device_id_type=MESH)

    @pl.when(even & gives_two)
    def _():
        pl.semaphore_wait(go_sem, 1)
        lax.fori_loop(0, inner, send_triangle, 0)


    def finish(step, scores):
        base = step * part

        @pl.when(odd)
        def _():
            own_copy(step).wait_recv()

        @pl.when(odd & has_two)
        def _():
            wait_two(step, RIGHT)
            pass_copy(step).start()
            for row in range(part):
                scores[row, 2 * breadth : 3 * breadth] = product(
                    far[base + row], enc[LEFT, base + row]
                )

        @pl.when(even & has_two)
        def _():
            pass_copy(step).wait_recv()

        def take_triangle():
            @pl.when(even & has_two)
            def _():
                tri_copy(step).wait_recv()
                unpack_triangle(step, scores)

        if scores is not held:
            take_triangle()
        for row in range(part):
            scores[row, :breadth] = product(enc[RIGHT, base + row], enc[LEFT, base + row])
            scores[row, breadth : 2 * breadth] = product(near[base + row], enc[LEFT, base + row])
            if scores is not held:
                b, h = place_of(step, row)
                volume_row(
                    scores, stage, out, row, b * height + h, span_count, level_count, scale
                )
        if scores is held:
            take_triangle()

    def finish_one(step, carry):
        finish(step, scores)
        return carry

    lax.fori_loop(0, inner, finish_one, 0)
    triangles(inner, chunks)
    lax.fori_loop(inner, chunks - 1, finish_one, 0)

    @pl.when(even)
    def _():
        sent(enc.at[RIGHT], near, 0, 1).wait_send()

    @pl.when(even & has_two)
    def _():
        sent(enc.at[LEFT], back, 1, -2, ahead).wait_send()

    for choice, when in sends_early:

        @pl.when(when)
        def _():
            for copy in sent_early(choice):
                copy.wait_send()

    for side in range(8):

        @pl.when(inside(*AROUND[side]))
        def _():
            halo_copy(side, pl.ds(0, 2)).wait_send()

    finish(chunks - 1, held)

    @pl.when(odd & has_two)
    def _():
        sent(far, near, 1, -1).wait_send()

    @pl.when(even & gives_two)
    def _():
        sent(tri_out, tri_in, 2, 2, rows=1).wait_send()

    @pl.when(odd & gives_two)
    def _():
        sent(enc.at[RIGHT], far, 0, 2, ahead).wait_send()


def store_kernel(batch, height, part, span_count, level_count, scale, done, held, out, tail, stage, sems):
    edge = part // 2
    last = (batch - 1) * height
    pieces = [(b * height + h, part) for b in range(batch - 1) for h in range(0, height, part)]
    pieces += [(last + h, part) for h in range(edge, height - edge, part)]
    copies = []
    for start, size in pieces:
        rows = pl.ds(start, size)
        copies.append(pltpu.make_async_copy(done.at[rows], out.at[rows], sems.at[len(copies)]))
    for copy in copies:
        copy.start()
    for half, start in enumerate((last, last + height - edge)):
        for row in range(half * edge, half * edge + edge):
            volume_row(held, stage, tail, row, row, span_count, level_count, scale)
        copies.append(
            pltpu.make_async_copy(
                tail.at[pl.ds(half * edge, edge)], out.at[pl.ds(start, edge)], sems.at[len(copies)]
            )
        )
        copies[-1].start()
    for copy in copies:
        copy.wait()


def in_hbm(array):
    return pltpu.with_memory_space_constraint(array, pltpu.HBM)


def shards(left_features, right_features, conv_weight, conv_bias):
    batch, height, breadth, channels = left_features.shape
    col_count = lax.axis_size("cols")
    part = math.gcd(height, 4)
    assert 2 * breadth == DISP and col_count % 2 == 0 and breadth % 32 == 0
    assert part % 2 == 0 and height > part
    lines = batch * height
    chunks = lines // part
    ahead = min(chunks - batch, 2)
    width = sum(DISP >> level for level in range(LEVELS))
    hbm = pl.BlockSpec(memory_space=pltpu.HBM)
    vmem = pl.BlockSpec(memory_space=pltpu.VMEM)
    dma = pltpu.SemaphoreType.DMA
    bf16, f32 = jnp.bfloat16, jnp.float32
    tri = (chunks, pl.cdiv(part * (breadth // 16) + part // 2, 2), 16, breadth)
    stage = pltpu.VMEM((part, 3, DISP + 16, breadth), f32)
    scale = 1.0 / math.sqrt(channels)
    done, held = pl.pallas_call(
        functools.partial(
            kernel, lax.axis_size("rows"), col_count, part, DISP, LEVELS, scale
        ),
        out_shape=[
            jax.ShapeDtypeStruct((lines, width, breadth), f32),
            jax.ShapeDtypeStruct((part, 3 * breadth, breadth), f32),
        ],
        in_specs=[hbm] * 4,
        out_specs=[vmem] * 2,
        scratch_shapes=[
            pltpu.VMEM((2, batch, height + 2, breadth, channels), bf16),
            pltpu.VMEM((part + 4, breadth, 2 * channels), bf16),
            pltpu.VMEM((2, 2, batch, height, 16, channels), bf16),
            pltpu.VMEM((2, 2, batch, height, 1, channels), f32),
            pltpu.VMEM((2, 2, batch, height + 2, 1, channels), f32),
            pltpu.VMEM((9 * channels, channels), bf16),
            pltpu.VMEM((1, channels), f32),
            pltpu.VMEM((2, lines, breadth, channels), bf16),
            pltpu.VMEM((ahead * part, breadth, channels), bf16),
            pltpu.VMEM((lines, breadth, channels), bf16),
            pltpu.VMEM((lines, breadth, channels), bf16),
            pltpu.VMEM((lines, breadth, channels), bf16),
            pltpu.VMEM(tri, bf16),
            pltpu.VMEM(tri, bf16),
            pltpu.VMEM((part, 3 * breadth, breadth), f32),
            stage,
            dma((4,)), dma((2, 2)), dma((8,)), dma((2, 8)), dma((ahead,)), dma((ahead,)),
            dma((5,)), dma((chunks,)), dma((chunks,)), dma((chunks,)), pltpu.SemaphoreType.REGULAR,
        ],
        compiler_params=pltpu.CompilerParams(
            collective_id=0, has_side_effects=True, vmem_limit_bytes=40 * 2**20
        ),
    )(
        in_hbm(left_features), in_hbm(right_features),
        in_hbm(conv_weight.reshape(9 * channels, channels)), in_hbm(conv_bias.reshape(1, -1)),
    )
    out = pl.pallas_call(
        functools.partial(store_kernel, batch, height, part, DISP, LEVELS, scale),
        out_shape=jax.ShapeDtypeStruct((lines, width, breadth), f32),
        in_specs=[vmem] * 2,
        out_specs=hbm,
        scratch_shapes=[
            pltpu.VMEM((part, width, breadth), f32), stage, dma((chunks + 1,)),
        ],
        compiler_params=pltpu.CompilerParams(vmem_limit_bytes=8 * 2**20),
    )(done, held)
    return jnp.swapaxes(out, 1, 2).reshape(batch, height, breadth, -1)


def solution(mesh):
    return jax.shard_map(
        shards,
        mesh=mesh,
        in_specs=(P(None, "rows", "cols", None), P(None, "rows", "cols", None), P(), P()),
        out_specs=P(None, "rows", "cols", None),
        check_vma=False,
    )
```

```python
import functools
import math

import jax
import jax.numpy as jnp
from jax import lax
from jax.experimental import pallas as pl
from jax.experimental.pallas import tpu as pltpu
from jax.sharding import PartitionSpec as P

DISP = 256
LEVELS = 4


MESH = pl.DeviceIdType.MESH
AROUND = ((-1, 0), (1, 0), (0, -1), (0, 1), (-1, -1), (-1, 1), (1, -1), (1, 1))
OPPOSITE = (1, 0, 3, 2, 7, 6, 5, 4)
ROW_SIDES = (0, 1)
COL_SIDES = (2, 3)
CORNERS = (4, 5, 6, 7)
LEFT, RIGHT = 0, 1
RIM = 16


def volume_row(scores, stage, out, slot, line, span_count, level_count, scale):
    breadth = scores.shape[2]
    steps = breadth - 1 - lax.broadcasted_iota(jnp.int32, (1, breadth), 1)
    bit = breadth // 2
    value = None
    while bit >= 8:
        keep = span_count + bit
        if value is None:
            low, high = scores[slot, :keep], scores[slot, bit : bit + keep]
        else:
            low, high = value[:keep], value[bit : bit + keep]
        value = jnp.where((steps & bit) != 0, high, low)
        bit //= 2
    for index, bit in enumerate((4, 2, 1)):
        keep = span_count + (8 if bit > 1 else 0)
        stage[slot, index, : span_count + 8] = value
        value = jnp.where((steps & bit) != 0, stage[slot, index, pl.ds(bit, keep)], value[:keep])
    out[line, :span_count] = value * scale
    start, size = 0, span_count
    for _ in range(1, level_count):
        half = size // 2
        pooled = (
            out[line, pl.ds(start, half, stride=2)] + out[line, pl.ds(start + 1, half, stride=2)]
        ) * 0.5
        start, size = start + size, half
        out[line, start : start + half] = pooled


def kernel(
    row_count, col_count, part, span_count, level_count, scale,
    left, right, weight_hbm, bias_hbm, out, held,
    images, sides, raw_edges, edges, col_halo, weight, bias, enc, early, near, far, back, tri_out, tri_in, scores, stage,
    in_sems, edge_sems, halo_sems, recv_sem, early_sems, rim_sems, send_sems, near_sems, two_sems, back_sems, go_sem,
):
    batch, height, breadth, channels = left.shape
    my_row, my_col = lax.axis_index("rows"), lax.axis_index("cols")
    edge = part // 2
    spans = height // part - 1
    chunks = batch * (spans + 1)
    inner = batch * spans
    ahead = min(inner, 2)

    def inside(step_row, step_col):
        row, col = my_row + step_row, my_col + step_col
        return (row >= 0) & (row < row_count) & (col >= 0) & (col < col_count)

    odd = lax.rem(my_col, 2) == 1
    even = jnp.logical_not(odd)
    has_two = my_col >= 2
    gives_two = my_col + 2 < col_count
    has_near = my_col >= 1
    first = jnp.where(gives_two, RIGHT, LEFT)
    second = 1 - first

    def fetch(image):
        source = right if image == RIGHT else left
        return pltpu.make_async_copy(
            source, images.at[image, :, pl.ds(1, height)], in_sems.at[image]
        )

    def fetch_edge(side, image):
        source = right if image == RIGHT else left
        return pltpu.make_async_copy(
            source.at[:, :, pl.ds(side * (breadth - 16), 16)],
            raw_edges.at[side, image], edge_sems.at[side, image],
        )

    def fetch_weight():
        return pltpu.make_async_copy(weight_hbm, weight, in_sems.at[2])

    def fetch_bias():
        return pltpu.make_async_copy(bias_hbm, bias, in_sems.at[3])

    barrier = pltpu.get_barrier_semaphore()
    partners = AROUND + ((0, -2), (0, 2))
    for step_row, step_col in partners:

        @pl.when(inside(step_row, step_col))
        def _():
            pl.semaphore_signal(
                barrier, inc=1, device_id=(my_row + step_row, my_col + step_col), device_id_type=MESH
            )

    for image in (RIGHT, LEFT):

        @pl.when(first == image)
        def _():
            for choice in (image, 1 - image):
                for side in range(2):
                    fetch_edge(side, choice).start()
            fetch(image).start()
            fetch_weight().start()
            fetch_bias().start()
            fetch(1 - image).start()

    def halo_copy(side, image):
        step_row, step_col = AROUND[side]
        if step_col == 0:
            source = images.at[image, :, 1 if step_row < 0 else height]
            target = images.at[image, :, height + 1 if step_row < 0 else 0]
        else:
            mine, theirs = (0, 1) if step_col < 0 else (1, 0)
            if step_row == 0:
                source = edges.at[mine, image]
                target = col_halo.at[theirs, image, :, pl.ds(1, height)]
            else:
                source = edges.at[mine, image, :, 0 if step_row < 0 else height - 1]
                target = col_halo.at[theirs, image, :, height + 1 if step_row < 0 else 0]
        return pltpu.make_async_remote_copy(
            src_ref=source, dst_ref=target,
            send_sem=halo_sems.at[side],
            recv_sem=recv_sem.at[OPPOSITE[side] + (8 if isinstance(image, int) and image else 0)],
            device_id=(my_row + step_row, my_col + step_col), device_id_type=MESH,
        )

    sends_early = ((RIGHT, odd & gives_two), (LEFT, even & has_two))

    def take_edges(image):
        for b in range(batch):
            for h in range(height):
                edges[0, image, b, h] = raw_edges[0, image, b, h].astype(jnp.float32)[0:1]
                edges[1, image, b, h] = raw_edges[1, image, b, h].astype(jnp.float32)[15:16]

    def send_halo(which, image):
        for side in which:

            @pl.when(inside(*AROUND[side]))
            def _():
                halo_copy(side, image).start()

    def wait_halo(which, image):
        for side in which:

            @pl.when(inside(*AROUND[OPPOSITE[side]]))
            def _():
                halo_copy(side, image).wait_recv()

    def clear_halo():
        for side in range(8):
            step_row, step_col = AROUND[side]

            @pl.when(jnp.logical_not(inside(step_row, step_col)))
            def _():
                line = 0 if step_row < 0 else height + 1
                for image in (LEFT, RIGHT):
                    for b in range(batch):
                        if step_col == 0:
                            images[image, b, line] = jnp.zeros((breadth, channels), jnp.bfloat16)
                        elif step_row == 0:
                            col_halo[0 if step_col < 0 else 1, image, b, pl.ds(1, height)] = jnp.zeros(
                                (height, 1, channels), jnp.float32
                            )
                        else:
                            col_halo[0 if step_col < 0 else 1, image, b, line] = jnp.zeros(
                                (1, channels), jnp.float32
                            )

    for image in (RIGHT, LEFT):

        @pl.when(first == image)
        def _():
            for side in range(2):
                fetch_edge(side, image).wait()

    take_edges(first)
    peers = sum(inside(*step).astype(jnp.int32) for step in partners)
    pl.semaphore_wait(barrier, peers)
    for image in (RIGHT, LEFT):

        @pl.when(first == image)
        def _():
            send_halo(COL_SIDES, image)
            for side in range(2):
                fetch_edge(side, 1 - image).wait()

    take_edges(second)
    for image in (RIGHT, LEFT):

        @pl.when(first == image)
        def _():
            send_halo(COL_SIDES, 1 - image)
            send_halo(CORNERS, pl.ds(0, 2))
            fetch(image).wait()
            send_halo(ROW_SIDES, image)
            fetch(1 - image).wait()
            send_halo(ROW_SIDES, 1 - image)

    clear_halo()

    @pl.when(jnp.logical_not(has_near))
    def _():
        near[...] = jnp.zeros_like(near)

    @pl.when(jnp.logical_not(has_two))
    def _():
        for target in (scores, held):
            target[:, 2 * breadth :] = jnp.zeros((part, breadth, breadth), jnp.float32)

    fetch_weight().wait()
    fetch_bias().wait()

    column = lax.broadcasted_iota(jnp.int32, (breadth, 1), 0)
    flip = jnp.where(
        lax.broadcasted_iota(jnp.int32, (breadth, breadth), 0)
        + lax.broadcasted_iota(jnp.int32, (breadth, breadth), 1)
        == breadth - 1,
        1.0, 0.0,
    ).astype(jnp.bfloat16)

    def place_of(step, row):
        is_inner = step < inner
        b = jnp.where(is_inner, step // spans, step - inner)
        h = jnp.where(
            is_inner,
            edge + lax.rem(step, spans) * part + row,
            row if row < edge else height - part + row,
        )
        return b, h

    def remote(source, target, send, recv, step, away, rows=part):
        lines = pl.ds(step * rows, rows)
        return pltpu.make_async_remote_copy(
            src_ref=source.at[lines], dst_ref=target.at[lines],
            send_sem=send_sems.at[send], recv_sem=recv.at[step],
            device_id=(my_row, my_col + away), device_id_type=MESH,
        )

    def own_copy(step):
        return remote(enc.at[RIGHT], near, 0, near_sems, step, 1)

    def far_copy(step):
        return remote(enc.at[RIGHT], far, 0, two_sems, step, 2)

    def pass_copy(step):
        return remote(far, near, 1, near_sems, step, -1)

    def back_copy(step):
        return remote(enc.at[LEFT], back, 1, back_sems, step, -2)

    def tri_copy(step):
        return remote(tri_out, tri_in, 2, two_sems, step, 2, 1)

    def toward_two(image):
        return (far, my_col + 2) if image == RIGHT else (back, my_col - 2)

    def early_copy(piece, image):
        target, col = toward_two(image)
        lines, pixels = pl.ds(piece * edge, edge), pl.ds(RIM, breadth - 2 * RIM)
        return pltpu.make_async_remote_copy(
            src_ref=early.at[lines, pixels], dst_ref=target.at[lines, pixels],
            send_sem=send_sems.at[3], recv_sem=early_sems.at[piece // 2],
            device_id=(my_row, col), device_id_type=MESH,
        )

    def rim_copy(step, side, image):
        target, col = toward_two(image)
        lines, pixels = pl.ds(step * part, part), pl.ds(side * (breadth - RIM), RIM)
        return pltpu.make_async_remote_copy(
            src_ref=enc.at[image, lines, pixels], dst_ref=target.at[lines, pixels],
            send_sem=send_sems.at[4], recv_sem=rim_sems.at[step],
            device_id=(my_row, col), device_id_type=MESH,
        )

    def wait_two(step, image):
        @pl.when(step < ahead)
        def _():
            for copy in arrived_early(step, image):
                copy.wait_recv()

        @pl.when(step >= ahead)
        def _():
            (far_copy if image == RIGHT else back_copy)(step).wait_recv()

    def start_two(step, image):
        @pl.when(step < ahead)
        def _():
            for side in range(2):
                rim_copy(step, side, image).start()

        @pl.when(step >= ahead)
        def _():
            (far_copy if image == RIGHT else back_copy)(step).start()

    def pieces_of(first_step, steps, image):
        target, col = toward_two(image)
        lines = pl.ds(first_step * part, steps * part)
        for send, recv, source, pixels in (
            (3, early_sems, early, pl.ds(RIM, breadth - 2 * RIM)),
            (4, rim_sems, enc.at[image], pl.ds(0, 2 * RIM)),
        ):
            yield pltpu.make_async_remote_copy(
                src_ref=source.at[lines, pixels], dst_ref=target.at[lines, pixels],
                send_sem=send_sems.at[send], recv_sem=recv.at[first_step],
                device_id=(my_row, col), device_id_type=MESH,
            )

    def arrived_early(step, image):
        return pieces_of(jnp.minimum(step, ahead - 1), 1, image)

    def sent_early(image):
        return pieces_of(0, ahead, image)

    def sent(source, target, send, away, low=0, high=chunks, rows=part):
        lines = pl.ds(low * rows, (high - low) * rows)
        return pltpu.make_async_remote_copy(
            src_ref=source.at[lines], dst_ref=target.at[lines],
            send_sem=send_sems.at[send], recv_sem=near_sems.at[0],
            device_id=(my_row, my_col + away), device_id_type=MESH,
        )

    def encoded(image, b, starts, count, bare):
        slots = count + 2
        rows = count * len(starts)
        for piece, start in enumerate(starts):
            for line in range(slots):
                row = images[image, b, start + line].astype(jnp.float32)
                before = 0.0 if bare else col_halo[0, image, b, start + line]
                after = 0.0 if bare else col_halo[1, image, b, start + line]
                sides[piece * slots + line, :, :channels] = jnp.where(
                    column == 0, before, pltpu.roll(row, 1, 0)
                ).astype(jnp.bfloat16)
                sides[piece * slots + line, :, channels:] = jnp.where(
                    column == breadth - 1, after, pltpu.roll(row, breadth - 1, 0)
                ).astype(jnp.bfloat16)

        def rows_from(offset):
            taken = [images[image, b, pl.ds(start + offset, count)] for start in starts]
            return jnp.concatenate(taken, axis=0).reshape(rows * breadth, channels)

        pieces = []
        for tap in range(3):
            beside = jnp.concatenate(
                [sides[i * slots + tap : i * slots + tap + count] for i in range(len(starts))], axis=0
            ).reshape(rows * breadth, 2 * channels)
            pieces += [beside[:, :channels], rows_from(tap), beside[:, channels:]]
        total = jnp.dot(
            jnp.concatenate(pieces, axis=1), weight[...], preferred_element_type=jnp.float32
        ) + bias[...]
        result = rows_from(1).astype(jnp.float32) + jnp.maximum(total, 0.0)
        return result.astype(jnp.bfloat16).reshape(rows, breadth, channels)

    def turned(plain):
        return jnp.dot(flip, plain, preferred_element_type=jnp.float32).astype(jnp.bfloat16)

    def convolve(image, step, b, starts, count):
        result = encoded(image, b, starts, count, False)
        base = step * part

        @pl.when(image == LEFT)
        def _():
            enc[LEFT, pl.ds(base, part)] = result

            @pl.when(even & has_two)
            def _():
                start_two(step, LEFT)

        @pl.when(image == RIGHT)
        def _():
            for row in range(part):
                enc[RIGHT, base + row] = turned(result[row])

            @pl.when(even)
            def _():
                own_copy(step).start()

            @pl.when(odd & gives_two)
            def _():
                start_two(step, RIGHT)

    def conv_early(piece, carry):
        step = piece // 2
        start = edge + lax.rem(step, spans) * part + lax.rem(piece, 2) * edge
        image = jnp.where(odd, RIGHT, LEFT)
        result = encoded(image, step // spans, [start], edge, True)

        @pl.when(odd)
        def _():
            for row in range(edge):
                early[piece * edge + row] = turned(result[row])
            early_copy(piece, RIGHT).start()

        @pl.when(even)
        def _():
            early[pl.ds(piece * edge, edge)] = result
            early_copy(piece, LEFT).start()

        return carry

    def conv_inner(image):
        def body(step, carry):
            convolve(image, step, step // spans, [edge + lax.rem(step, spans) * part], part)
            return carry

        lax.fori_loop(0, inner, body, 0)

    def conv_edge(image):
        def body(step, carry):
            convolve(image, step, step - inner, [0, height - edge], edge)
            return carry

        lax.fori_loop(inner, chunks, body, 0)

    def both(act, image):
        for choice in (RIGHT, LEFT):

            @pl.when(image == choice)
            def _():
                act(choice)

    def product(keys, queries):
        return lax.dot_general(
            keys, queries, (((1,), (1,)), ((), ())), preferred_element_type=jnp.float32
        )

    half_blocks = breadth // 16
    lane8 = lax.broadcasted_iota(jnp.int32, (8, breadth), 1)

    def triangle(step, carry):
        base = step * part
        wait_two(step, LEFT)
        packed, middles = [], []
        for row in range(part):
            block = product(enc[RIGHT, base + row], back[base + row])
            packed.append(block[0:8])
            for i in range(1, half_blocks):
                cut = breadth - 8 * i
                packed.append(
                    jnp.where(
                        lane8 < cut, block[8 * i : 8 * i + 8], pltpu.roll(block[cut : cut + 8], cut, 1)
                    )
                )
            middles.append(block[8 * half_blocks : 8 * half_blocks + 8])
        for row in range(0, part, 2):
            packed.append(
                jnp.where(
                    lane8 < breadth // 2, middles[row], pltpu.roll(middles[row + 1], breadth // 2, 1)
                )
            )
        packed += packed[: len(packed) % 2]
        for i in range(len(packed) // 2):
            tile = jnp.concatenate(packed[2 * i : 2 * i + 2], axis=0)
            tri_out[step, i] = tile.astype(jnp.bfloat16)

        @pl.when(step >= inner)
        def _():
            tri_copy(step).start()

        return carry

    def unpack_triangle(step, scores):
        def packed(index):
            tile = tri_in[step, index // 2].astype(jnp.float32)
            return tile[8 * (index % 2) : 8 * (index % 2) + 8]

        def put(row, block_row, block):
            start = 2 * breadth + 8 * block_row
            scores[row, start : start + 8] = block

        for row in range(part):
            for i in range(half_blocks):
                block = packed(row * half_blocks + i)
                put(row, i, block)
                if i > 0:
                    put(row, 2 * half_blocks - i, pltpu.roll(block, 8 * i, 1))
            block = packed(part * half_blocks + row // 2)
            put(row, half_blocks, block if row % 2 == 0 else pltpu.roll(block, breadth // 2, 1))

    def send_triangle(step, carry):
        tri_copy(step).start()
        return carry

    def triangles(low, high):
        @pl.when(even & gives_two)
        def _():
            lax.fori_loop(low, high, triangle, 0)

    @pl.when((odd & gives_two) | (even & has_two))
    def _():
        lax.fori_loop(0, 2 * ahead, conv_early, 0)

    both(functools.partial(wait_halo, COL_SIDES), first)
    conv_inner(first)
    both(functools.partial(wait_halo, COL_SIDES), second)
    conv_inner(second)
    both(functools.partial(wait_halo, ROW_SIDES), first)
    wait_halo(CORNERS, pl.ds(0, 2))
    conv_edge(first)
    triangles(0, inner)
    both(functools.partial(wait_halo, ROW_SIDES), second)
    conv_edge(second)

    @pl.when(odd & gives_two)
    def _():
        pl.semaphore_signal(go_sem, inc=1, device_id=(my_row, my_col - 1), device_id_type=MESH)

    @pl.when(even & gives_two)
    def _():
        pl.semaphore_wait(go_sem, 1)
        lax.fori_loop(0, inner, send_triangle, 0)


    def finish(step, scores):
        base = step * part

        @pl.when(odd)
        def _():
            own_copy(step).wait_recv()

        @pl.when(odd & has_two)
        def _():
            wait_two(step, RIGHT)
            pass_copy(step).start()
            for row in range(part):
                scores[row, 2 * breadth : 3 * breadth] = product(
                    far[base + row], enc[LEFT, base + row]
                )

        @pl.when(even & has_two)
        def _():
            pass_copy(step).wait_recv()

        def take_triangle():
            @pl.when(even & has_two)
            def _():
                tri_copy(step).wait_recv()
                unpack_triangle(step, scores)

        if scores is not held:
            take_triangle()
        for row in range(part):
            scores[row, :breadth] = product(enc[RIGHT, base + row], enc[LEFT, base + row])
            scores[row, breadth : 2 * breadth] = product(near[base + row], enc[LEFT, base + row])
            if scores is not held:
                b, h = place_of(step, row)
                volume_row(
                    scores, stage, out, row, b * height + h, span_count, level_count, scale
                )
        if scores is held:
            take_triangle()

    def finish_one(step, carry):
        finish(step, scores)
        return carry

    lax.fori_loop(0, inner, finish_one, 0)
    triangles(inner, chunks)
    lax.fori_loop(inner, chunks - 1, finish_one, 0)

    @pl.when(even)
    def _():
        sent(enc.at[RIGHT], near, 0, 1).wait_send()

    @pl.when(even & has_two)
    def _():
        sent(enc.at[LEFT], back, 1, -2, ahead).wait_send()

    for choice, when in sends_early:

        @pl.when(when)
        def _():
            for copy in sent_early(choice):
                copy.wait_send()

    for side in range(8):

        @pl.when(inside(*AROUND[side]))
        def _():
            halo_copy(side, pl.ds(0, 2)).wait_send()

    finish(chunks - 1, held)

    @pl.when(odd & has_two)
    def _():
        sent(far, near, 1, -1).wait_send()

    @pl.when(even & gives_two)
    def _():
        sent(tri_out, tri_in, 2, 2, rows=1).wait_send()

    @pl.when(odd & gives_two)
    def _():
        sent(enc.at[RIGHT], far, 0, 2, ahead).wait_send()


def store_kernel(batch, height, part, span_count, level_count, scale, done, held, out, tail, stage, sems):
    edge = part // 2
    last = (batch - 1) * height
    pieces = [(b * height + h, part) for b in range(batch - 1) for h in range(0, height, part)]
    pieces += [(last + h, part) for h in range(edge, height - edge, part)]
    copies = []
    for start, size in pieces:
        rows = pl.ds(start, size)
        copies.append(pltpu.make_async_copy(done.at[rows], out.at[rows], sems.at[len(copies)]))
    for copy in copies:
        copy.start()
    for half, start in enumerate((last, last + height - edge)):
        for row in range(half * edge, half * edge + edge):
            volume_row(held, stage, tail, row, row, span_count, level_count, scale)
        copies.append(
            pltpu.make_async_copy(
                tail.at[pl.ds(half * edge, edge)], out.at[pl.ds(start, edge)], sems.at[len(copies)]
            )
        )
        copies[-1].start()
    for copy in copies:
        copy.wait()


def in_hbm(array):
    return pltpu.with_memory_space_constraint(array, pltpu.HBM)


def shards(left_features, right_features, conv_weight, conv_bias):
    batch, height, breadth, channels = left_features.shape
    col_count = lax.axis_size("cols")
    part = math.gcd(height, 4)
    assert 2 * breadth == DISP and col_count % 2 == 0 and breadth % 32 == 0
    assert part % 2 == 0 and height > part
    lines = batch * height
    chunks = lines // part
    ahead = min(chunks - batch, 2)
    width = sum(DISP >> level for level in range(LEVELS))
    hbm = pl.BlockSpec(memory_space=pltpu.HBM)
    vmem = pl.BlockSpec(memory_space=pltpu.VMEM)
    dma = pltpu.SemaphoreType.DMA
    bf16, f32 = jnp.bfloat16, jnp.float32
    tri = (chunks, pl.cdiv(part * (breadth // 16) + part // 2, 2), 16, breadth)
    stage = pltpu.VMEM((part, 3, DISP + 16, breadth), f32)
    scale = 1.0 / math.sqrt(channels)
    done, held = pl.pallas_call(
        functools.partial(
            kernel, lax.axis_size("rows"), col_count, part, DISP, LEVELS, scale
        ),
        out_shape=[
            jax.ShapeDtypeStruct((lines, width, breadth), f32),
            jax.ShapeDtypeStruct((part, 3 * breadth, breadth), f32),
        ],
        in_specs=[hbm] * 4,
        out_specs=[vmem] * 2,
        scratch_shapes=[
            pltpu.VMEM((2, batch, height + 2, breadth, channels), bf16),
            pltpu.VMEM((part + 4, breadth, 2 * channels), bf16),
            pltpu.VMEM((2, 2, batch, height, 16, channels), bf16),
            pltpu.VMEM((2, 2, batch, height, 1, channels), f32),
            pltpu.VMEM((2, 2, batch, height + 2, 1, channels), f32),
            pltpu.VMEM((9 * channels, channels), bf16),
            pltpu.VMEM((1, channels), f32),
            pltpu.VMEM((2, lines, breadth, channels), bf16),
            pltpu.VMEM((ahead * part, breadth, channels), bf16),
            pltpu.VMEM((lines, breadth, channels), bf16),
            pltpu.VMEM((lines, breadth, channels), bf16),
            pltpu.VMEM((lines, breadth, channels), bf16),
            pltpu.VMEM(tri, bf16),
            pltpu.VMEM(tri, bf16),
            pltpu.VMEM((part, 3 * breadth, breadth), f32),
            stage,
            dma((4,)), dma((2, 2)), dma((8,)), dma((12,)), dma((ahead,)), dma((ahead,)),
            dma((5,)), dma((chunks,)), dma((chunks,)), dma((chunks,)), pltpu.SemaphoreType.REGULAR,
        ],
        compiler_params=pltpu.CompilerParams(
            collective_id=0, has_side_effects=True, vmem_limit_bytes=40 * 2**20
        ),
    )(
        in_hbm(left_features), in_hbm(right_features),
        in_hbm(conv_weight.reshape(9 * channels, channels)), in_hbm(conv_bias.reshape(1, -1)),
    )
    out = pl.pallas_call(
        functools.partial(store_kernel, batch, height, part, DISP, LEVELS, scale),
        out_shape=jax.ShapeDtypeStruct((lines, width, breadth), f32),
        in_specs=[vmem] * 2,
        out_specs=hbm,
        scratch_shapes=[
            pltpu.VMEM((part, width, breadth), f32), stage, dma((chunks + 1,)),
        ],
        compiler_params=pltpu.CompilerParams(vmem_limit_bytes=8 * 2**20),
    )(done, held)
    return jnp.swapaxes(out, 1, 2).reshape(batch, height, breadth, -1)


def solution(mesh):
    return jax.shard_map(
        shards,
        mesh=mesh,
        in_specs=(P(None, "rows", "cols", None), P(None, "rows", "cols", None), P(), P()),
        out_specs=P(None, "rows", "cols", None),
        check_vma=False,
    )
```
